256 devices in a mesh: dp: 32 (over x, y, core), adapter: 8 (over z).
Axes of the slice: x: 4, y: 4, z: 8, core: 2. Of those that a mesh axis runs over, the one named last changes fastest.
Arguments:
- tokens: bfloat16 [32768, 1024], P('dp'), may hold values from -60 to 60
- down_weight: bfloat16 [16, 1024, 64], P('adapter'), may hold values from -0.1875 to 0.1875
- down_bias: bfloat16 [16, 64], P('adapter'), may hold values from -3 to 3
- up_weight: bfloat16 [16, 64, 1024], P('adapter'), may hold values from -0.75 to 0.75
- up_bias: bfloat16 [16, 1024], P('adapter'), may hold values from -3 to 3
- query_weight: bfloat16 [1024, 1024], P(('dp', 'adapter')), may hold values from -0.1875 to 0.1875
- key_weight: bfloat16 [1024, 1024], P(('dp', 'adapter')), may hold values from -0.1875 to 0.1875
- value_weight: bfloat16 [1024, 1024], P(('dp', 'adapter')), may hold values from -0.1875 to 0.1875
Outputs:
- united_out: bfloat16 [32768, 1024], P(('dp', 'adapter'))
The draws below stay inside these ranges and needn't reach their ends.
All inputs are finite; a program needn't handle non-finite values.
Results may differ from the reference program's by a relative error of at most 0.012.
The reference program's roundings to bfloat16 on the way count: a program that leaves them out, or rounds other values in their place, can miss the bound.
Values may be sent and summed in bfloat16 or wider, within the bound.
A program may use at most 64 MiB of HBM per device.

```python
import math
import jax
import jax.numpy as jnp
from jax import lax

D = 1024
R = 64
TOK_DEV = 1024
ADAPTERS = 16
N_DP = 32


def draw_tokens(key, part):
    base_key = jax.random.fold_in(key, 11)
    normal_key, scale_key = jax.random.split(base_key)
    values = jnp.clip(jax.random.normal(normal_key, (TOK_DEV * N_DP, D), jnp.float32), -6.0, 6.0)
    return values.astype(jnp.bfloat16)


def levels(own_key, dims, cuts, smallest, top_value):
    loudness, own = 1.0, jax.random.fold_in(own_key, 6)
    for position, parts in cuts:
        draws = jnp.exp(jax.random.uniform(jax.random.fold_in(own, position), (parts,), jnp.float32, smallest / len(cuts), top_value / len(cuts)))
        loudness = loudness * jnp.repeat(draws, dims[position] // parts).reshape([-1 if axis == position else 1 for axis in range(len(dims))])
    return loudness


def normal_values(stream_key, dims, deviation, most, cuts=(), kind=jnp.bfloat16):
    loudness = levels(stream_key, dims, cuts, -0.22, 0.18) if cuts else 1.0
    result = jax.random.normal(stream_key, dims, jnp.float32) * deviation * loudness
    return jnp.minimum(jnp.maximum(result, -most), most).astype(kind)


def setup_inputs(seed: int = 0) -> dict:
    key_list = jax.random.split(jax.random.key(seed), 9)
    tokens = draw_tokens(jax.random.fold_in(key_list[8], 71), 0)
    down_weight = normal_values(key_list[1], (ADAPTERS, D, R), D ** -0.5, 0.1875, ((0, 8),))
    down_bias = normal_values(key_list[2], (ADAPTERS, R), 0.5, 3.0, ((0, 8),))
    up_weight = normal_values(key_list[3], (ADAPTERS, R, D), R ** -0.5, 0.75, ((0, 8),))
    up_bias = normal_values(key_list[4], (ADAPTERS, D), 0.5, 3.0, ((0, 8),))
    query_weight = normal_values(key_list[5], (D, D), D ** -0.5, 0.1875, ((0, 256),))
    key_weight = normal_values(key_list[6], (D, D), D ** -0.5, 0.1875, ((0, 256),))
    value_weight = normal_values(key_list[7], (D, D), D ** -0.5, 0.1875, ((0, 256),))
    return {"tokens": tokens, "down_weight": down_weight, "down_bias": down_bias, "up_weight": up_weight, "up_bias": up_bias, "query_weight": query_weight, "key_weight": key_weight, "value_weight": value_weight}


def reference(tokens, down_weight, down_bias, up_weight, up_bias, query_weight, key_weight, value_weight):
    score_scale = 1.0 / math.sqrt(D)
    tok_rows = tokens.shape[0]
    query_rows = jnp.dot(tokens, query_weight, preferred_element_type=jnp.float32)
    tok_float = tokens.astype(jnp.float32)

    def absorb(state_in, adapter_item):
        peak, denominator, summed = state_in
        down_block, down_shift, up_block, up_shift = adapter_item
        hidden = jax.nn.relu(jnp.dot(tokens, down_block, preferred_element_type=jnp.float32) + down_shift.astype(jnp.float32)[None, :]).astype(jnp.bfloat16)
        adapted = (tok_float + jnp.dot(hidden, up_block, preferred_element_type=jnp.float32) + up_shift.astype(jnp.float32)[None, :]).astype(jnp.bfloat16)
        key_rows = jnp.dot(adapted, key_weight, preferred_element_type=jnp.float32)
        value_rows = jnp.dot(adapted, value_weight, preferred_element_type=jnp.float32)
        scores = lax.optimization_barrier(jnp.sum(query_rows * key_rows, axis=1)) * score_scale
        new_peak = jnp.maximum(peak, scores)
        keep_old = jnp.exp(peak - new_peak)
        fresh = jnp.exp(scores - new_peak)
        denominator = denominator * keep_old + fresh
        summed = summed * keep_old[:, None] + fresh[:, None] * value_rows
        return ((new_peak, denominator, summed), None)
    start_state = (jnp.full((tok_rows,), -jnp.inf, jnp.float32), jnp.zeros((tok_rows,), jnp.float32), jnp.zeros((tok_rows, D), jnp.float32))
    (peak, denominator, summed), _ = lax.scan(absorb, start_state, (down_weight, down_bias, up_weight, up_bias))
    united = summed / denominator[:, None]
    return (tok_float + united).astype(jnp.bfloat16)
```

```python
import functools

import jax
import jax.numpy as jnp
from jax import lax
from jax.experimental import pallas as pl
from jax.experimental.pallas import tpu as pltpu
from jax.sharding import PartitionSpec as P

BF16, F32 = jnp.bfloat16, jnp.float32
NX, NY, NC, NZ = 4, 4, 2, 8
Z_STEPS = (4, 3, -3, 2, -2, 1, -1)
NT = (((1,), (1,)), ((), ()))


class Copy:
    def __init__(self, name, region, step, needs, size, front=0.0):
        self.name, self.region, self.step = name, region, step
        self.needs, self.size, self.front = needs, size, front


class Work:
    def __init__(self, name, run, needs, cost):
        self.name, self.run, self.needs, self.cost = name, run, needs, cost


def plan_copies():
    copies = {}

    def add(name, region, step, needs, size, front=0.0):
        copies[name] = Copy(name, region, step, tuple(needs), size, front)

    def page(m):
        return lambda r, x, y, c, z: r["w"].at[m, x, y, c, pl.ds(4 * z, 4)]

    for m in range(3):
        for d in Z_STEPS:
            add(("page", m, d), page(m), (0, 0, 0, d), (), 8)
    for d in Z_STEPS:
        add(("ub", d), lambda r, x, y, c, z: r["ub"].at[z], (0, 0, 0, d), (), 4)
        add(("db", d), lambda r, x, y, c, z: r["db"].at[z], (0, 0, 0, d), (), 1)

    def ring(buf, back):
        return lambda r, x, y, c, z: r[buf].at[(z + back + NZ) % NZ, c]

    for s in range(1, 5):
        for buf, way in (("dn", 1), ("up", -1), ("up", 1), ("dn", -1)):
            if s == 4 and (buf, way) in (("up", 1), ("dn", -1)):
                continue
            needs = [("ring", buf, way, s - 1)] if s > 1 else []
            add(("ring", buf, way, s), ring(buf, -way * (s - 1)), (0, 0, 0, way), needs, 128)
    for buf in ("dn", "up"):
        for k in (-1, 1, -2, 2, -3, 3, 4):
            src = ("ring", buf, 1, -k) if k < 0 else ("ring", buf, -1, k)
            if k == 4 and buf == "dn":
                src = ("ring", "dn", 1, 4)
            add(("pair", buf, k), ring(buf, k), (0, 0, 1, 0), [src], 128)

    def block(m, h, i, j, lo, rows):
        def at(r, x, y, c, z):
            a, b = (x, y) if h == 0 else (y, x)
            a, b = (a + i + 4) % 4, (b + j + 4) % 4
            x, y = (a, b) if h == 0 else (b, a)
            return r["w"].at[m, x, y, c, pl.ds(16 * h + lo, rows)]

        return at

    def line(m, h, j, lo, rows):
        def at(r, x, y, c, z):
            if h == 0:
                return r["w"].at[m, :, (y + j + 4) % 4, c, pl.ds(16 * h + lo, rows)]
            return r["w"].at[m, (x + j + 4) % 4, :, c, pl.ds(16 * h + lo, rows)]

        return at

    for m in range(3):
        mine = [("page", m, d) for d in Z_STEPS]
        for h in range(2):
            along = (lambda d: (d, 0, 0, 0)) if h == 0 else (lambda d: (0, d, 0, 0))
            across = (lambda d: (0, d, 0, 0)) if h == 0 else (lambda d: (d, 0, 0, 0))
            key = (m, h)
            for d in (1, -1):
                add(("s1", key, d), block(m, h, 0, 0, 0, 16), along(d), mine, 32)
                add(("s3", key, 0, d), block(m, h, 0, 0, 0, 16), across(d), mine, 32)
            for d in (1, -1):
                lo = 0 if d == 1 else 8
                add(("s2", key, d), block(m, h, -d, 0, lo, 8), along(d), [("s1", key, d)], 16)
            for i in (-1, 1, 2):
                src = [("s1", key, -i)] if i != 2 else [("s2", key, 1), ("s2", key, -1)]
                for d in (1, -1):
                    add(("s3", key, i, d), block(m, h, i, 0, 0, 16), across(d), src, 32)
            for d in (1, -1):
                lo = 0 if d == 1 else 8
                got = [("s3", key, i, d) for i in (0, -1, 1, 2)]
                add(("s4", key, d), line(m, h, -d, lo, 8), across(d), got, 64)
            add(
                ("hand", key, 0),
                line(m, h, 0, 0, 16),
                (0, 0, 1, 0),
                mine + [("s1", key, 1), ("s1", key, -1), ("s2", key, 1), ("s2", key, -1)],
                128,
            )
            for d in (1, -1):
                got = [("s3", key, i, d) for i in (0, -1, 1, 2)]
                add(("hand", key, -d), line(m, h, -d, 0, 16), (0, 0, 1, 0), got, 128)
            add(("hand", key, 2), line(m, h, 2, 0, 16), (0, 0, 1, 0), [("s4", key, 1), ("s4", key, -1)], 128)
    return copies


def all_of(m):
    names = [("page", m, d) for d in Z_STEPS]
    for h in range(2):
        key = (m, h)
        names += [("s1", key, d) for d in (1, -1)] + [("s2", key, d) for d in (1, -1)]
        names += [("s3", key, i, d) for i in (0, -1, 1, 2) for d in (1, -1)]
        names += [("s4", key, d) for d in (1, -1)]
        names += [("hand", key, j) for j in (0, 1, -1, 2)]
    return names


def pair_needs(k):
    if k == 0:
        return []
    d = -k if k != 4 else 4
    names = [("ub", d), ("db", d), ("pair", "dn", k), ("pair", "up", k)]
    for buf in ("dn", "up"):
        src = ("ring", buf, 1, -k) if k < 0 else ("ring", buf, -1, k)
        if k == 4 and buf == "dn":
            src = ("ring", "dn", 1, 4)
        names.append(src)
    return names


def plan_order(copies, works):
    free, arrival, order = {}, {}, []
    now, waited, done = 0.0, set(), set()
    unsent, todo = list(copies), list(works)
    while True:
        moved = True
        while moved:
            moved = False
            for name in list(unsent):
                c = copies[name]
                if all(n in waited for n in c.needs):
                    axis = next(i for i in range(4) if c.step[i])
                    hops = abs(c.step[axis])
                    if axis == 2:
                        link, rate, late = "core", 620.0, 0.9
                    else:
                        link, rate, late = (axis, c.step[axis] > 0), 45.0, 0.95 + 0.8 * hops
                    begin = max(now, free.get(link, 0.0))
                    took = c.size * 1.024 / rate * hops
                    free[link] = begin + took
                    arrival[name] = begin + took + late
                    order.append(("start", name))
                    unsent.remove(name)
                    now += 0.01
                    moved = True
        ready = sorted((t, i, n) for i, (n, t) in enumerate(arrival.items()) if n not in waited)
        if ready and ready[0][0] <= now:
            order.append(("wait", ready[0][2]))
            waited.add(ready[0][2])
            continue
        run = next((w for w in todo if all(n in waited or n in done for n in w.needs)), None)
        if run is not None:
            order.append(("work", run.name))
            now += run.cost
            done.add(run.name)
            todo.remove(run)
            continue
        if not ready:
            break
        now = ready[0][0]
    assert not unsent and not todo
    return order, now


def kernel(
    copies, tokens, dn_in, db_in, up_in, ub_in, q_in, k_in, v_in, out, xs, w, dn, up, db, ub, ad, qhl, qk, mix, loc, ss, rs
):
    dp, z = lax.axis_index("dp"), lax.axis_index("adapter")
    x, y, c = dp // 8, (dp // 2) % 4, dp % 2
    refs = {"w": w, "dn": dn, "up": up, "db": db, "ub": ub}
    ids = {name: i for i, name in enumerate(copies)}

    own = [
        (q_in, w.at[0, x, y, c, pl.ds(4 * z, 4)]),
        (k_in, w.at[1, x, y, c, pl.ds(4 * z, 4)]),
        (v_in, w.at[2, x, y, c, pl.ds(4 * z, 4)]),
        (ub_in, ub.at[z]),
        (db_in, db.at[z]),
        (dn_in, dn.at[z]),
        (up_in, up.at[z]),
        (tokens.at[pl.ds(128 * z, 128)], xs),
    ]
    own = [pltpu.make_async_copy(a, b, loc.at[i]) for i, (a, b) in enumerate(own)]
    for cp in own:
        cp.start()

    def there(step, sign):
        px, py, pz = (x + sign * step[0] + 4) % 4, (y + sign * step[1] + 4) % 4, (z + sign * step[3] + NZ) % NZ
        pc = 1 - c if step[2] else c
        return px, py, pc, pz

    def device(step):
        px, py, pc, pz = there(step, 1)
        return ((px * NY + py) * NC + pc, pz)

    def descriptor(name, sender):
        cp = copies[name]
        region = cp.region(refs, *sender)
        i = ids[name]
        return pltpu.make_async_remote_copy(
            src_ref=region,
            dst_ref=region,
            send_sem=ss.at[i],
            recv_sem=rs.at[i],
            device_id=device(cp.step),
            device_id_type=pl.DeviceIdType.MESH,
        )

    peers = [(0, 0, 0, d) for d in Z_STEPS] + [(1, 0, 0, 0), (-1, 0, 0, 0), (0, 1, 0, 0), (0, -1, 0, 0), (0, 0, 1, 0)]
    barrier = pltpu.get_barrier_semaphore()
    for step in peers:
        pl.semaphore_signal(barrier, inc=1, device_id=device(step), device_id_type=pl.DeviceIdType.MESH)
    pl.semaphore_wait(barrier, len(peers))
    for cp in own:
        cp.wait()

    def adapters(k):
        def run():
            at = (z + k + NZ) % NZ
            bias = db[at].astype(F32)
            bias = jnp.concatenate([bias[0:1], bias[1:2]], axis=1)
            hid = lax.dot_general(xs[...], dn[at].reshape(128, 1024), NT, preferred_element_type=F32)
            hid = jnp.maximum(hid + bias, 0.0).astype(BF16)
            lift = ub[at].astype(F32)
            for i in range(2):
                for n in range(4):
                    cols = slice(256 * n, 256 * n + 256)
                    raised = jnp.dot(hid[:, 64 * i : 64 * i + 64], up[at, i, :, cols], preferred_element_type=F32)
                    ad[2 * ((k + NZ) % NZ) + i, :, cols] = (
                        xs[:, cols].astype(F32) + raised + lift[i : i + 1, cols]
                    ).astype(BF16)

        return run

    def split(part, rows, cols, value):
        high = value.astype(BF16)
        part[rows, cols] = high
        low = slice(rows.start + 128, rows.stop + 128) if isinstance(rows, slice) else rows
        part[low, cols] = (value - high.astype(F32)).astype(BF16)

    def query():
        whole = w.at[0].reshape(1024, 1024)
        for n in range(4):
            cols = slice(256 * n, 256 * n + 256)
            split(qhl, slice(0, 128), cols, jnp.dot(xs[...], whole[:, cols], preferred_element_type=F32))

    def key():
        whole = w.at[1].reshape(1024, 1024)
        for n in range(4):
            cols = slice(256 * n, 256 * n + 256)
            both = lax.dot_general(qhl[...], whole[cols, :], NT, preferred_element_type=F32)
            qk[:, cols] = (both[:128] + both[128:]) * (1.0 / 32.0)

    def attend():
        @pl.loop(0, 8)
        def _(step):
            rows = pl.ds(pl.multiple_of(step * 16, 16), 16)
            weight = qk[rows, :]
            scores = [jnp.sum(ad[a, rows, :].astype(F32) * weight, axis=1, keepdims=True) for a in range(16)]
            peak = functools.reduce(jnp.maximum, scores)
            scores = [jnp.exp(s - peak) for s in scores]
            scale = 1.0 / functools.reduce(jnp.add, scores)
            total = scores[0] * ad[0, rows, :].astype(F32)
            for a in range(1, 16):
                total = total + scores[a] * ad[a, rows, :].astype(F32)
            total = total * scale
            high = total.astype(BF16)
            mix[rows, :] = high
            mix[pl.ds(pl.multiple_of(step * 16 + 128, 16), 16), :] = (total - high.astype(F32)).astype(BF16)

    def value():
        whole = w.at[2].reshape(1024, 1024)
        for n in range(4):
            cols = slice(256 * n, 256 * n + 256)
            both = jnp.dot(mix[...], whole[:, cols], preferred_element_type=F32)
            out[:, cols] = (xs[:, cols].astype(F32) + both[:128] + both[128:]).astype(BF16)

    works = [
        Work("q", query, all_of(0), 0.6),
        Work("k", key, ["q"] + all_of(1), 0.8),
    ]
    pairs = [0, -1, 1, -2, 2, -3, 3, 4]
    works += [Work(("a", k), adapters(k), pair_needs(k), 0.6) for k in pairs]
    works.append(Work("s", attend, ["k"] + [("a", k) for k in pairs], 3.0))
    works.append(Work("v", value, ["s"] + all_of(2), 0.8))
    by_name = {job.name: job for job in works}
    order, _ = plan_order(copies, works)
    for kind, name in order:
        if kind == "start":
            descriptor(name, (x, y, c, z)).start()
        elif kind == "wait":
            descriptor(name, there(copies[name].step, -1)).wait_recv()
        else:
            by_name[name].run()
    for name in copies:
        descriptor(name, (x, y, c, z)).wait_send()


def body(tokens, down_weight, down_bias, up_weight, up_bias, query_weight, key_weight, value_weight):
    copies = plan_copies()
    hbm = pl.BlockSpec(memory_space=pl.ANY)
    return pl.pallas_call(
        functools.partial(kernel, copies),
        out_shape=jax.ShapeDtypeStruct((128, 1024), BF16),
        in_specs=[hbm] * 8,
        out_specs=pl.BlockSpec(memory_space=pltpu.VMEM),
        scratch_shapes=[
            pltpu.VMEM((128, 1024), BF16),
            pltpu.VMEM((3, NX, NY, NC, 32, 1024), BF16),
            pltpu.VMEM((NZ, 2, 64, 1024), BF16),
            pltpu.VMEM((NZ, 2, 64, 1024), BF16),
            pltpu.VMEM((NZ, 2, 64), BF16),
            pltpu.VMEM((NZ, 2, 1024), BF16),
            pltpu.VMEM((16, 128, 1024), BF16),
            pltpu.VMEM((256, 1024), BF16),
            pltpu.VMEM((128, 1024), F32),
            pltpu.VMEM((256, 1024), BF16),
            pltpu.SemaphoreType.DMA((8,)),
            pltpu.SemaphoreType.DMA((len(copies),)),
            pltpu.SemaphoreType.DMA((len(copies),)),
        ],
        compiler_params=pltpu.CompilerParams(
            collective_id=0, has_side_effects=True, vmem_limit_bytes=48 * 1024 * 1024
        ),
    )(
        tokens,
        jnp.swapaxes(down_weight, 1, 2),
        down_bias,
        up_weight,
        up_bias,
        query_weight,
        key_weight,
        value_weight,
    )


def solution(mesh):
    in_specs = (
        P("dp", None),
        P("adapter", None, None),
        P("adapter", None),
        P("adapter", None, None),
        P("adapter", None),
        P(("dp", "adapter"), None),
        P(("dp", "adapter"), None),
        P(("dp", "adapter"), None),
    )
    out_specs = P(("dp", "adapter"), None)
    return jax.shard_map(body, mesh=mesh, in_specs=in_specs, out_specs=out_specs, check_vma=False)
```

```python
import functools

import jax
import jax.numpy as jnp
from jax import lax
from jax.experimental import pallas as pl
from jax.experimental.pallas import tpu as pltpu
from jax.sharding import PartitionSpec as P

BF16, F32 = jnp.bfloat16, jnp.float32
NX, NY, NC, NZ = 4, 4, 2, 8
Z_STEPS = (4, 3, -3, 2, -2, 1, -1)
NT = (((1,), (1,)), ((), ()))


class Copy:
    def __init__(self, name, region, step, needs, size):
        self.name, self.region, self.step = name, region, step
        self.needs, self.size = needs, size


class Work:
    def __init__(self, name, run, needs, cost):
        self.name, self.run, self.needs, self.cost = name, run, needs, cost


def up_from(k):
    if k == 4:
        return [("up", 0, 1, 4), ("up", 1, -1, 4)]
    way = 1 if k < 0 else -1
    return [("up", half, way, abs(k)) for half in range(2)]


def plan_copies():
    copies = {}

    def add(name, region, step, needs, size):
        copies[name] = Copy(name, region, step, tuple(needs), size)

    def reach(name, region, size, way):
        for d in (2, -2, 1, -1):
            add((*name, d), region(0), (0, 0, 0, d), (), size)
        for d in (3, -3):
            sign = d // 3
            add((*name, d), region(-2 * sign), (0, 0, 0, sign), [(*name, 2 * sign)], size)
        add((*name, 4), region(-2 * way), (0, 0, 0, 2 * way), [(*name, 2 * way)], size)

    def page(m):
        return lambda back: lambda r, x, y, c, z: r["w"].at[m, x, y, c, pl.ds(4 * ((z + back + NZ) % NZ), 4)]

    for m in range(3):
        reach(("page", m), page(m), 8, (1, -1, 1)[m])
    reach(("ub",), lambda back: lambda r, x, y, c, z: r["ub"].at[(z + back + NZ) % NZ], 4, -1)

    def ring(half, back):
        return lambda r, x, y, c, z: r["up"].at[(z + back + NZ) % NZ, c, pl.ds(32 * half, 32)]

    for s in range(1, 5):
        for half, way in ((0, 1), (1, -1), (1, 1), (0, -1)):
            if s == 4 and (half, way) in ((1, 1), (0, -1)):
                continue
            needs = [("up", half, way, s - 1)] if s > 1 else []
            add(("up", half, way, s), ring(half, -way * (s - 1)), (0, 0, 0, way), needs, 64)

    def hidden(src, dst, lo, rows):
        return lambda r, x, y, c, z: r["hb"].at[(z + src + NZ) % NZ, (z + dst + NZ) % NZ, pl.ds(lo, rows)]

    for sign in (1, -1):
        lo = 0 if sign == 1 else 64
        add(("hop", 4, lo), hidden(0, 4, lo, 64), (0, 0, 0, 2 * sign), ["h"], 16)
        add(("hop", 3 * sign), hidden(0, 3 * sign, 0, 128), (0, 0, 0, 2 * sign), ["h"], 32)
    for sign in (1, -1):
        for d in (2, 1):
            add(("hid", d * sign), hidden(0, d * sign, 0, 128), (0, 0, 0, d * sign), ["h"], 32)
    for sign in (1, -1):
        lo = 0 if sign == 1 else 64
        add(("hid", 3 * sign), hidden(-2 * sign, sign, 0, 128), (0, 0, 0, sign), [("hop", 3 * sign)], 32)
        add(("hid", 4, lo), hidden(-2 * sign, 2 * sign, lo, 64), (0, 0, 0, 2 * sign), [("hop", 4, lo)], 16)

    def whole(k):
        return lambda r, x, y, c, z: r["up"].at[(z + k + NZ) % NZ, c]

    for k in (-1, 1, -2, 2, -3, 3, 4):
        add(("pair", k), whole(k), (0, 0, 1, 0), up_from(k), 128)

    def block(m, h, i, j, lo, rows):
        def at(r, x, y, c, z):
            a, b = (x, y) if h == 0 else (y, x)
            a, b = (a + i + 4) % 4, (b + j + 4) % 4
            x, y = (a, b) if h == 0 else (b, a)
            return r["w"].at[m, x, y, c, pl.ds(16 * h + lo, rows)]

        return at

    def line(m, h, j, lo, rows):
        def at(r, x, y, c, z):
            if h == 0:
                return r["w"].at[m, :, (y + j + 4) % 4, c, pl.ds(16 * h + lo, rows)]
            return r["w"].at[m, (x + j + 4) % 4, :, c, pl.ds(16 * h + lo, rows)]

        return at

    for m in range(3):
        mine = [("page", m, d) for d in Z_STEPS]
        for h in range(2):
            along = (lambda d: (d, 0, 0, 0)) if h == 0 else (lambda d: (0, d, 0, 0))
            across = (lambda d: (0, d, 0, 0)) if h == 0 else (lambda d: (d, 0, 0, 0))
            key = (m, h)
            for d in (1, -1):
                add(("s1", key, d), block(m, h, 0, 0, 0, 16), along(d), mine, 32)
                add(("s3", key, 0, d), block(m, h, 0, 0, 0, 16), across(d), mine, 32)
            for d in (1, -1):
                lo = 0 if d == 1 else 8
                add(("s2", key, d), block(m, h, -d, 0, lo, 8), along(d), [("s1", key, d)], 16)
            for i in (-1, 1, 2):
                src = [("s1", key, -i)] if i != 2 else [("s2", key, 1), ("s2", key, -1)]
                for d in (1, -1):
                    add(("s3", key, i, d), block(m, h, i, 0, 0, 16), across(d), src, 32)
            for d in (1, -1):
                lo = 0 if d == 1 else 8
                got = [("s3", key, i, d) for i in (0, -1, 1, 2)]
                add(("s4", key, d), line(m, h, -d, lo, 8), across(d), got, 64)
            add(
                ("hand", key, 0),
                line(m, h, 0, 0, 16),
                (0, 0, 1, 0),
                mine + [("s1", key, 1), ("s1", key, -1), ("s2", key, 1), ("s2", key, -1)],
                128,
            )
            for d in (1, -1):
                got = [("s3", key, i, d) for i in (0, -1, 1, 2)]
                add(("hand", key, -d), line(m, h, -d, 0, 16), (0, 0, 1, 0), got, 128)
            for d in (1, -1):
                lo = 0 if d == 1 else 8
                add(("hand", key, 2, d), line(m, h, 2, lo, 8), (0, 0, 1, 0), [("s4", key, d)], 64)
    return copies


def all_of(m):
    names = [("page", m, d) for d in Z_STEPS]
    for h in range(2):
        key = (m, h)
        names += [("s1", key, d) for d in (1, -1)] + [("s2", key, d) for d in (1, -1)]
        names += [("s3", key, i, d) for i in (0, -1, 1, 2) for d in (1, -1)]
        names += [("s4", key, d) for d in (1, -1)]
        names += [("hand", key, j) for j in (0, 1, -1)] + [("hand", key, 2, d) for d in (1, -1)]
    return names


def pair_needs(k):
    if k == 0:
        return ["h"]
    hid = [("hid", 4, 0), ("hid", 4, 64)] if k == 4 else [("hid", -k)]
    return [("ub", 4 if k == 4 else -k), ("pair", k), *hid, *up_from(k)]


def plan_order(copies, works):
    free, arrival, order = {}, {}, []
    now, waited, done = 0.0, set(), set()
    unsent, todo = list(copies), list(works)
    while True:
        moved = True
        while moved:
            moved = False
            for name in list(unsent):
                c = copies[name]
                if all(n in waited or n in done for n in c.needs):
                    axis = next(i for i in range(4) if c.step[i])
                    hops = abs(c.step[axis])
                    if axis == 2:
                        link, rate, late = "core", 620.0, 0.9
                    else:
                        link, rate, late = (axis, c.step[axis] > 0), 41.0, 0.95 + 0.8 * hops
                    begin = max(now, free.get(link, 0.0))
                    took = c.size * 1.024 / rate * hops
                    free[link] = begin + took
                    arrival[name] = begin + took + late
                    order.append(("start", name))
                    unsent.remove(name)
                    now += 0.01
                    moved = True
        ready = sorted((t, i, n) for i, (n, t) in enumerate(arrival.items()) if n not in waited)
        if ready and ready[0][0] <= now:
            order.append(("wait", ready[0][2]))
            waited.add(ready[0][2])
            continue
        run = next((w for w in todo if all(n in waited or n in done for n in w.needs)), None)
        if run is not None:
            order.append(("work", run.name))
            now += run.cost
            done.add(run.name)
            todo.remove(run)
            continue
        if not ready:
            break
        now = ready[0][0]
    assert not unsent and not todo
    return order, now


def kernel(
    copies, tokens, dn_in, db_in, up_in, ub_in, q_in, k_in, v_in, out, xa, xs, w, dn, up, db, ub, hb, ad, qhl, qk, sc, mix, loc, ss, rs
):
    dp, z = lax.axis_index("dp"), lax.axis_index("adapter")
    x, y, c = dp // 8, (dp // 2) % 4, dp % 2
    refs = {"w": w, "up": up, "ub": ub, "hb": hb}
    ids = {name: i for i, name in enumerate(copies)}

    own = [
        (q_in, w.at[0, x, y, c, pl.ds(4 * z, 4)]),
        (k_in, w.at[1, x, y, c, pl.ds(4 * z, 4)]),
        (v_in, w.at[2, x, y, c, pl.ds(4 * z, 4)]),
        (ub_in, ub.at[z]),
        (up_in, up.at[z]),
        (db_in, db),
        (dn_in, dn),
        (tokens, xa),
        (tokens.at[pl.ds(128 * z, 128)], xs),
    ]
    own = [pltpu.make_async_copy(a, b, loc.at[i]) for i, (a, b) in enumerate(own)]
    for cp in own:
        cp.start()

    def there(step, sign):
        px, py, pz = (x + sign * step[0] + 4) % 4, (y + sign * step[1] + 4) % 4, (z + sign * step[3] + NZ) % NZ
        pc = 1 - c if step[2] else c
        return px, py, pc, pz

    def device(step):
        px, py, pc, pz = there(step, 1)
        return ((px * NY + py) * NC + pc, pz)

    def descriptor(name, sender):
        cp = copies[name]
        region = cp.region(refs, *sender)
        i = ids[name]
        return pltpu.make_async_remote_copy(
            src_ref=region,
            dst_ref=region,
            send_sem=ss.at[i],
            recv_sem=rs.at[i],
            device_id=device(cp.step),
            device_id_type=pl.DeviceIdType.MESH,
        )

    peers = [(0, 0, 0, d) for d in (1, -1, 2, -2)] + [(1, 0, 0, 0), (-1, 0, 0, 0), (0, 1, 0, 0), (0, -1, 0, 0), (0, 0, 1, 0)]
    barrier = pltpu.get_barrier_semaphore()
    for step in peers:
        pl.semaphore_signal(barrier, inc=1, device_id=device(step), device_id_type=pl.DeviceIdType.MESH)
    pl.semaphore_wait(barrier, len(peers))
    for cp in own:
        cp.wait()

    def hide():
        bias = db[...].astype(F32)
        bias = jnp.concatenate([bias[0:1], bias[1:2]], axis=1)
        both = dn.reshape(128, 1024)

        @pl.loop(0, NZ)
        def _(to):
            rows = xa[pl.ds(pl.multiple_of(to * 128, 128), 128), :]
            raised = lax.dot_general(rows, both[...], NT, preferred_element_type=F32)
            hb[z, to] = jnp.maximum(raised + bias, 0.0).astype(BF16)

    def adapters(k):
        def run():
            at = (z + k + NZ) % NZ
            hid = hb[at, z]
            lift = ub[at].astype(F32)
            for i in range(2):
                for n in range(4):
                    cols = slice(256 * n, 256 * n + 256)
                    raised = jnp.dot(hid[:, 64 * i : 64 * i + 64], up[at, i, :, cols], preferred_element_type=F32)
                    ad[2 * ((k + NZ) % NZ) + i, :, cols] = (
                        xs[:, cols].astype(F32) + raised + lift[i : i + 1, cols]
                    ).astype(BF16)

        return run

    def score(k):
        def run():
            first = 2 * ((k + NZ) % NZ)

            @pl.loop(0, 8)
            def _(step):
                rows = pl.ds(pl.multiple_of(step * 16, 16), 16)
                weight = qk[rows, :]
                for a in (first, first + 1):
                    sc[a, rows, :] = jnp.sum(ad[a, rows, :].astype(F32) * weight, axis=1, keepdims=True)

        return run

    def split(part, rows, cols, value):
        high = value.astype(BF16)
        part[rows, cols] = high
        low = slice(rows.start + 128, rows.stop + 128) if isinstance(rows, slice) else rows
        part[low, cols] = (value - high.astype(F32)).astype(BF16)

    def query():
        whole = w.at[0].reshape(1024, 1024)
        for n in range(4):
            cols = slice(256 * n, 256 * n + 256)
            split(qhl, slice(0, 128), cols, jnp.dot(xs[...], whole[:, cols], preferred_element_type=F32))

    def key():
        whole = w.at[1].reshape(1024, 1024)
        for n in range(4):
            cols = slice(256 * n, 256 * n + 256)
            both = lax.dot_general(qhl[...], whole[cols, :], NT, preferred_element_type=F32)
            qk[:, cols] = (both[:128] + both[128:]) * (1.0 / 32.0)

    def attend():
        @pl.loop(0, 8)
        def _(step):
            rows = pl.ds(pl.multiple_of(step * 16, 16), 16)
            scores = [sc[a, rows, :] for a in range(16)]
            peak = functools.reduce(jnp.maximum, scores)
            scores = [jnp.exp(s - peak) for s in scores]
            scale = 1.0 / functools.reduce(jnp.add, scores)
            total = scores[0] * ad[0, rows, :].astype(F32)
            for a in range(1, 16):
                total = total + scores[a] * ad[a, rows, :].astype(F32)
            total = total * scale
            high = total.astype(BF16)
            mix[rows, :] = high
            mix[pl.ds(pl.multiple_of(step * 16 + 128, 16), 16), :] = (total - high.astype(F32)).astype(BF16)

    def value():
        whole = w.at[2].reshape(1024, 1024)
        for n in range(4):
            cols = slice(256 * n, 256 * n + 256)
            both = jnp.dot(mix[...], whole[:, cols], preferred_element_type=F32)
            out[:, cols] = (xs[:, cols].astype(F32) + both[:128] + both[128:]).astype(BF16)

    pairs = [0, -1, 1, -2, 2, -3, 3, 4]
    works = [Work("h", hide, [], 1.3), Work("q", query, all_of(0), 0.6), Work("k", key, ["q"] + all_of(1), 0.8)]
    works += [Work(("a", k), adapters(k), pair_needs(k), 0.5) for k in pairs]
    works += [Work(("s", k), score(k), ["k", ("a", k)], 0.3) for k in pairs]
    works.append(Work("m", attend, [("s", k) for k in pairs], 1.5))
    works.append(Work("v", value, ["m"] + all_of(2), 0.8))
    by_name = {job.name: job for job in works}
    order, _ = plan_order(copies, works)
    for kind, name in order:
        if kind == "start":
            descriptor(name, (x, y, c, z)).start()
        elif kind == "wait":
            descriptor(name, there(copies[name].step, -1)).wait_recv()
        else:
            by_name[name].run()
    for name in copies:
        descriptor(name, (x, y, c, z)).wait_send()


def body(tokens, down_weight, down_bias, up_weight, up_bias, query_weight, key_weight, value_weight):
    copies = plan_copies()
    hbm = pl.BlockSpec(memory_space=pltpu.HBM)
    return pl.pallas_call(
        functools.partial(kernel, copies),
        out_shape=jax.ShapeDtypeStruct((128, 1024), BF16),
        in_specs=[hbm] * 8,
        out_specs=pl.BlockSpec(memory_space=pltpu.VMEM),
        scratch_shapes=[
            pltpu.VMEM((1024, 1024), BF16),
            pltpu.VMEM((128, 1024), BF16),
            pltpu.VMEM((3, NX, NY, NC, 32, 1024), BF16),
            pltpu.VMEM((2, 64, 1024), BF16),
            pltpu.VMEM((NZ, 2, 64, 1024), BF16),
            pltpu.VMEM((2, 64), BF16),
            pltpu.VMEM((NZ, 2, 1024), BF16),
            pltpu.VMEM((NZ, NZ, 128, 128), BF16),
            pltpu.VMEM((16, 128, 1024), BF16),
            pltpu.VMEM((256, 1024), BF16),
            pltpu.VMEM((128, 1024), F32),
            pltpu.VMEM((16, 128, 1), F32),
            pltpu.VMEM((256, 1024), BF16),
            pltpu.SemaphoreType.DMA((9,)),
            pltpu.SemaphoreType.DMA((len(copies),)),
            pltpu.SemaphoreType.DMA((len(copies),)),
        ],
        compiler_params=pltpu.CompilerParams(
            collective_id=0, has_side_effects=True, vmem_limit_bytes=67043328
        ),
    )(
        tokens,
        jnp.swapaxes(down_weight, 1, 2),
        down_bias,
        up_weight,
        up_bias,
        query_weight,
        key_weight,
        value_weight,
    )


def solution(mesh):
    in_specs = (
        P("dp", None),
        P("adapter", None, None),
        P("adapter", None),
        P("adapter", None, None),
        P("adapter", None),
        P(("dp", "adapter"), None),
        P(("dp", "adapter"), None),
        P(("dp", "adapter"), None),
    )
    out_specs = P(("dp", "adapter"), None)
    return jax.shard_map(body, mesh=mesh, in_specs=in_specs, out_specs=out_specs, check_vma=False)
```

```python
import functools

import jax
import jax.numpy as jnp
from jax import lax
from jax.experimental import pallas as pl
from jax.experimental.pallas import tpu as pltpu
from jax.sharding import PartitionSpec as P

BF16, F32 = jnp.bfloat16, jnp.float32
NX, NY, NC, NZ = 4, 4, 2, 8
Z_STEPS = (4, 3, -3, 2, -2, 1, -1)
NT = (((1,), (1,)), ((), ()))


class Copy:
    def __init__(self, name, region, step, needs, size):
        self.name, self.region, self.step = name, region, step
        self.needs, self.size = needs, size


class Work:
    def __init__(self, name, run, needs, cost):
        self.name, self.run, self.needs, self.cost = name, run, needs, cost


def up_from(k):
    if k == 4:
        return [("up", 0, 1, 4), ("up", 1, -1, 4)]
    way = 1 if k < 0 else -1
    return [("up", half, way, abs(k)) for half in range(2)]


def plan_copies():
    copies = {}

    def add(name, region, step, needs, size):
        copies[name] = Copy(name, region, step, tuple(needs), size)

    def reach(name, region, size, way):
        for d in (2, -2, 1, -1):
            add((*name, d), region(0), (0, 0, 0, d), (), size)
        for d in (3, -3):
            sign = d // 3
            add((*name, d), region(-2 * sign), (0, 0, 0, sign), [(*name, 2 * sign)], size)
        add((*name, 4), region(-2 * way), (0, 0, 0, 2 * way), [(*name, 2 * way)], size)

    def page(m):
        return lambda back: lambda r, x, y, c, z: r["w"].at[m, x, y, c, pl.ds(4 * ((z + back + NZ) % NZ), 4)]

    for m in range(3):
        reach(("page", m), page(m), 8, (1, -1, 1)[m])
    reach(("ub",), lambda back: lambda r, x, y, c, z: r["ub"].at[(z + back + NZ) % NZ], 4, -1)

    def ring(half, back):
        return lambda r, x, y, c, z: r["up"].at[(z + back + NZ) % NZ, c, pl.ds(32 * half, 32)]

    for s in range(1, 5):
        for half, way in ((0, 1), (1, -1), (1, 1), (0, -1)):
            if s == 4 and (half, way) in ((1, 1), (0, -1)):
                continue
            needs = [("up", half, way, s - 1)] if s > 1 else []
            add(("up", half, way, s), ring(half, -way * (s - 1)), (0, 0, 0, way), needs, 64)

    def hidden(src, dst, lo, rows):
        return lambda r, x, y, c, z: r["hb"].at[(z + src + NZ) % NZ, (z + dst + NZ) % NZ, pl.ds(lo, rows)]

    for sign in (1, -1):
        lo = 0 if sign == 1 else 64
        add(("hop", 4, lo), hidden(0, 4, lo, 64), (0, 0, 0, 2 * sign), ["h"], 16)
        add(("hop", 3 * sign), hidden(0, 3 * sign, 0, 128), (0, 0, 0, 2 * sign), ["h"], 32)
    for sign in (1, -1):
        for d in (2, 1):
            add(("hid", d * sign), hidden(0, d * sign, 0, 128), (0, 0, 0, d * sign), ["h"], 32)
    for sign in (1, -1):
        lo = 0 if sign == 1 else 64
        add(("hid", 3 * sign), hidden(-2 * sign, sign, 0, 128), (0, 0, 0, sign), [("hop", 3 * sign)], 32)
        add(("hid", 4, lo), hidden(-2 * sign, 2 * sign, lo, 64), (0, 0, 0, 2 * sign), [("hop", 4, lo)], 16)

    def whole(k):
        return lambda r, x, y, c, z: r["up"].at[(z + k + NZ) % NZ, c]

    for k in (-1, 1, -2, 2, -3, 3, 4):
        add(("pair", k), whole(k), (0, 0, 1, 0), up_from(k), 128)

    def block(m, h, i, j, lo, rows):
        def at(r, x, y, c, z):
            a, b = (x, y) if h == 0 else (y, x)
            a, b = (a + i + 4) % 4, (b + j + 4) % 4
            x, y = (a, b) if h == 0 else (b, a)
            return r["w"].at[m, x, y, c, pl.ds(16 * h + lo, rows)]

        return at

    def line(m, h, j, lo, rows):
        def at(r, x, y, c, z):
            if h == 0:
                return r["w"].at[m, :, (y + j + 4) % 4, c, pl.ds(16 * h + lo, rows)]
            return r["w"].at[m, (x + j + 4) % 4, :, c, pl.ds(16 * h + lo, rows)]

        return at

    for m in range(3):
        mine = [("page", m, d) for d in Z_STEPS]
        for h in range(2):
            along = (lambda d: (d, 0, 0, 0)) if h == 0 else (lambda d: (0, d, 0, 0))
            across = (lambda d: (0, d, 0, 0)) if h == 0 else (lambda d: (d, 0, 0, 0))
            key = (m, h)
            for d in (1, -1):
                add(("s1", key, d), block(m, h, 0, 0, 0, 16), along(d), mine, 32)
                add(("s3", key, 0, d), block(m, h, 0, 0, 0, 16), across(d), mine, 32)
            for d in (1, -1):
                lo = 0 if d == 1 else 8
                add(("s2", key, d), block(m, h, -d, 0, lo, 8), along(d), [("s1", key, d)], 16)
            for i in (-1, 1, 2):
                src = [("s1", key, -i)] if i != 2 else [("s2", key, 1), ("s2", key, -1)]
                for d in (1, -1):
                    add(("s3", key, i, d), block(m, h, i, 0, 0, 16), across(d), src, 32)
            for d in (1, -1):
                lo = 0 if d == 1 else 8
                got = [("s3", key, i, d) for i in (0, -1, 1, 2)]
                add(("s4", key, d), line(m, h, -d, lo, 8), across(d), got, 64)
            add(
                ("hand", key, 0),
                line(m, h, 0, 0, 16),
                (0, 0, 1, 0),
                mine + [("s1", key, 1), ("s1", key, -1), ("s2", key, 1), ("s2", key, -1)],
                128,
            )
            for d in (1, -1):
                got = [("s3", key, i, d) for i in (0, -1, 1, 2)]
                add(("hand", key, -d), line(m, h, -d, 0, 16), (0, 0, 1, 0), got, 128)
            for d in (1, -1):
                lo = 0 if d == 1 else 8
                add(("hand", key, 2, d), line(m, h, 2, lo, 8), (0, 0, 1, 0), [("s4", key, d)], 64)
    return copies


def all_of(m):
    names = [("page", m, d) for d in Z_STEPS]
    for h in range(2):
        key = (m, h)
        names += [("s1", key, d) for d in (1, -1)] + [("s2", key, d) for d in (1, -1)]
        names += [("s3", key, i, d) for i in (0, -1, 1, 2) for d in (1, -1)]
        names += [("s4", key, d) for d in (1, -1)]
        names += [("hand", key, j) for j in (0, 1, -1)] + [("hand", key, 2, d) for d in (1, -1)]
    return names


def pair_needs(k):
    if k == 0:
        return ["h"]
    hid = [("hid", 4, 0), ("hid", 4, 64)] if k == 4 else [("hid", -k)]
    return [("ub", 4 if k == 4 else -k), ("pair", k), *hid, *up_from(k)]


def urgency(name):
    kind = name[0]
    if kind == "page":
        return (0, name[1], 0)
    if kind in ("ub", "up", "hop", "hid", "pair"):
        return (1, {"hop": 0, "up": 1, "hid": 2, "ub": 3, "pair": 4}[kind], 0)
    return (2 + name[1][0], {"s1": 0, "s2": 1, "s3": 2, "s4": 3, "hand": 4}[kind], 0)


def plan_order(copies, works, backlog=2.0):
    free, arrival, order = {}, {}, []
    now, waited, done = 0.0, set(), set()
    unsent, todo = sorted(copies, key=urgency), list(works)

    def route(c):
        axis = next(i for i in range(4) if c.step[i])
        hops = abs(c.step[axis])
        if axis == 2:
            return "core", c.size / 600.0, 0.9
        return (axis, c.step[axis] > 0), c.size * hops / 41.0, 0.95 + 0.8 * hops

    def start_ready(until):
        nonlocal now
        for name in list(unsent):
            c = copies[name]
            if all(n in waited or n in done for n in c.needs):
                link, took, late = route(c)
                if free.get(link, 0.0) - until > backlog:
                    continue
                begin = max(now, free.get(link, 0.0))
                free[link] = begin + took
                arrival[name] = begin + took + late
                order.append(("start", name))
                unsent.remove(name)
                now += 0.01

    while True:
        start_ready(now)
        ready = sorted((t, i, n) for i, (n, t) in enumerate(arrival.items()) if n not in waited)
        if ready and ready[0][0] <= now:
            order.append(("wait", ready[0][2]))
            waited.add(ready[0][2])
            continue
        run = next((w for w in todo if all(n in waited or n in done for n in w.needs)), None)
        if run is not None:
            order.append(("work", run.name))
            now += run.cost
            done.add(run.name)
            todo.remove(run)
            continue
        if not ready:
            break
        start_ready(ready[0][0])
        ready = sorted((t, i, n) for i, (n, t) in enumerate(arrival.items()) if n not in waited)
        now = max(now, ready[0][0])
    assert not unsent and not todo
    return order, now


def kernel(
    copies, tokens, dn_in, db_in, up_in, ub_in, q_in, k_in, v_in, out, xa, xs, w, dn, up, db, ub, hb, ad, qhl, qk, sc, mix, loc, ss, rs
):
    dp, z = lax.axis_index("dp"), lax.axis_index("adapter")
    x, y, c = dp // 8, (dp // 2) % 4, dp % 2
    refs = {"w": w, "up": up, "ub": ub, "hb": hb}
    ids = {name: i for i, name in enumerate(copies)}

    own = [
        (q_in, w.at[0, x, y, c, pl.ds(4 * z, 4)]),
        (k_in, w.at[1, x, y, c, pl.ds(4 * z, 4)]),
        (v_in, w.at[2, x, y, c, pl.ds(4 * z, 4)]),
        (ub_in, ub.at[z]),
        (up_in, up.at[z]),
        (db_in, db),
        (dn_in, dn),
        (tokens, xa),
        (tokens.at[pl.ds(128 * z, 128)], xs),
    ]
    own = [pltpu.make_async_copy(a, b, loc.at[i]) for i, (a, b) in enumerate(own)]
    for cp in own:
        cp.start()

    def there(step, sign):
        px, py, pz = (x + sign * step[0] + 4) % 4, (y + sign * step[1] + 4) % 4, (z + sign * step[3] + NZ) % NZ
        pc = 1 - c if step[2] else c
        return px, py, pc, pz

    def device(step):
        px, py, pc, pz = there(step, 1)
        return ((px * NY + py) * NC + pc, pz)

    def descriptor(name, sender):
        cp = copies[name]
        region = cp.region(refs, *sender)
        i = ids[name]
        return pltpu.make_async_remote_copy(
            src_ref=region,
            dst_ref=region,
            send_sem=ss.at[i],
            recv_sem=rs.at[i],
            device_id=device(cp.step),
            device_id_type=pl.DeviceIdType.MESH,
        )

    peers = [(0, 0, 0, d) for d in (1, -1, 2, -2)] + [(1, 0, 0, 0), (-1, 0, 0, 0), (0, 1, 0, 0), (0, -1, 0, 0), (0, 0, 1, 0)]
    barrier = pltpu.get_barrier_semaphore()
    for step in peers:
        pl.semaphore_signal(barrier, inc=1, device_id=device(step), device_id_type=pl.DeviceIdType.MESH)
    pl.semaphore_wait(barrier, len(peers))
    for cp in own[:5]:
        cp.wait()

    def hide():
        for cp in own[5:]:
            cp.wait()
        bias = db[...].astype(F32)
        bias = jnp.concatenate([bias[0:1], bias[1:2]], axis=1)
        both = dn.reshape(128, 1024)

        @pl.loop(0, NZ)
        def _(to):
            rows = xa[pl.ds(pl.multiple_of(to * 128, 128), 128), :]
            raised = lax.dot_general(rows, both[...], NT, preferred_element_type=F32)
            hb[z, to] = jnp.maximum(raised + bias, 0.0).astype(BF16)

    def adapters(k):
        def run():
            at = (z + k + NZ) % NZ
            hid = hb[at, z]
            lift = ub[at].astype(F32)
            for i in range(2):
                for n in range(4):
                    cols = slice(256 * n, 256 * n + 256)
                    raised = jnp.dot(hid[:, 64 * i : 64 * i + 64], up[at, i, :, cols], preferred_element_type=F32)
                    ad[2 * ((k + NZ) % NZ) + i, :, cols] = (
                        xs[:, cols].astype(F32) + raised + lift[i : i + 1, cols]
                    ).astype(BF16)

        return run

    def score(k):
        def run():
            first = 2 * ((k + NZ) % NZ)
            for a in (first, first + 1):
                total = ad[a, :, :128].astype(F32) * qk[:, :128]
                for n in range(1, 8):
                    cols = slice(128 * n, 128 * n + 128)
                    total = total + ad[a, :, cols].astype(F32) * qk[:, cols]
                sc[:, a : a + 1] = jnp.sum(total, axis=1, keepdims=True)

        return run

    def split(part, rows, cols, value):
        high = value.astype(BF16)
        part[rows, cols] = high
        low = slice(rows.start + 128, rows.stop + 128) if isinstance(rows, slice) else rows
        part[low, cols] = (value - high.astype(F32)).astype(BF16)

    def query():
        whole = w.at[0].reshape(1024, 1024)
        for n in range(4):
            cols = slice(256 * n, 256 * n + 256)
            split(qhl, slice(0, 128), cols, jnp.dot(xs[...], whole[:, cols], preferred_element_type=F32))

    def key():
        whole = w.at[1].reshape(1024, 1024)
        for n in range(4):
            cols = slice(256 * n, 256 * n + 256)
            both = lax.dot_general(qhl[...], whole[cols, :], NT, preferred_element_type=F32)
            qk[:, cols] = (both[:128] + both[128:]) * (1.0 / 32.0)

    def attend():
        weight = sc[:, :16]
        weight = jnp.exp(weight - jnp.max(weight, axis=1, keepdims=True))
        weight = weight / jnp.sum(weight, axis=1, keepdims=True)
        for row in range(0, 128, 16):
            rows = slice(row, row + 16)
            total = weight[rows, :1] * ad[0, rows, :].astype(F32)
            for a in range(1, 16):
                total = total + weight[rows, a : a + 1] * ad[a, rows, :].astype(F32)
            split(mix, rows, slice(None), total)

    def value():
        whole = w.at[2].reshape(1024, 1024)
        for n in range(4):
            cols = slice(256 * n, 256 * n + 256)
            both = jnp.dot(mix[...], whole[:, cols], preferred_element_type=F32)
            out[:, cols] = (xs[:, cols].astype(F32) + both[:128] + both[128:]).astype(BF16)

    pairs = [0, -1, 1, -2, 2, -3, 3, 4]
    works = [Work("h", hide, [], 1.3), Work("q", query, all_of(0), 0.6), Work("k", key, ["q"] + all_of(1), 0.8)]
    works += [Work(("a", k), adapters(k), pair_needs(k), 0.5) for k in pairs]
    works += [Work(("s", k), score(k), ["k", ("a", k)], 0.3) for k in pairs]
    works.append(Work("m", attend, [("s", k) for k in pairs], 1.5))
    works.append(Work("v", value, ["m"] + all_of(2), 0.8))
    by_name = {job.name: job for job in works}
    order, _ = plan_order(copies, works)
    for kind, name in order:
        if kind == "start":
            descriptor(name, (x, y, c, z)).start()
        elif kind == "wait":
            descriptor(name, there(copies[name].step, -1)).wait_recv()
        else:
            by_name[name].run()
    for name in copies:
        descriptor(name, (x, y, c, z)).wait_send()


def body(tokens, down_weight, down_bias, up_weight, up_bias, query_weight, key_weight, value_weight):
    copies = plan_copies()
    hbm = pl.BlockSpec(memory_space=pltpu.HBM)
    return pl.pallas_call(
        functools.partial(kernel, copies),
        out_shape=jax.ShapeDtypeStruct((128, 1024), BF16),
        in_specs=[hbm] * 8,
        out_specs=pl.BlockSpec(memory_space=pltpu.VMEM),
        scratch_shapes=[
            pltpu.VMEM((1024, 1024), BF16),
            pltpu.VMEM((128, 1024), BF16),
            pltpu.VMEM((3, NX, NY, NC, 32, 1024), BF16),
            pltpu.VMEM((2, 64, 1024), BF16),
            pltpu.VMEM((NZ, 2, 64, 1024), BF16),
            pltpu.VMEM((2, 64), BF16),
            pltpu.VMEM((NZ, 2, 1024), BF16),
            pltpu.VMEM((NZ, NZ, 128, 128), BF16),
            pltpu.VMEM((16, 128, 1024), BF16),
            pltpu.VMEM((256, 1024), BF16),
            pltpu.VMEM((128, 1024), F32),
            pltpu.VMEM((128, 16), F32),
            pltpu.VMEM((256, 1024), BF16),
            pltpu.SemaphoreType.DMA((9,)),
            pltpu.SemaphoreType.DMA((len(copies),)),
            pltpu.SemaphoreType.DMA((len(copies),)),
        ],
        compiler_params=pltpu.CompilerParams(
            collective_id=0, has_side_effects=True, vmem_limit_bytes=67043328
        ),
    )(
        tokens,
        jnp.swapaxes(down_weight, 1, 2),
        down_bias,
        up_weight,
        up_bias,
        query_weight,
        key_weight,
        value_weight,
    )


def solution(mesh):
    in_specs = (
        P("dp", None),
        P("adapter", None, None),
        P("adapter", None),
        P("adapter", None, None),
        P("adapter", None),
        P(("dp", "adapter"), None),
        P(("dp", "adapter"), None),
        P(("dp", "adapter"), None),
    )
    out_specs = P(("dp", "adapter"), None)
    return jax.shard_map(body, mesh=mesh, in_specs=in_specs, out_specs=out_specs, check_vma=False)
```

```python
import functools

import jax
import jax.numpy as jnp
from jax import lax
from jax.experimental import pallas as pl
from jax.experimental.pallas import tpu as pltpu
from jax.sharding import PartitionSpec as P

BF16, F32 = jnp.bfloat16, jnp.float32
NX, NY, NC, NZ = 4, 4, 2, 8
Z_STEPS = (4, 3, -3, 2, -2, 1, -1)
NT = (((1,), (1,)), ((), ()))


class Copy:
    def __init__(self, name, region, step, needs, size):
        self.name, self.region, self.step = name, region, step
        self.needs, self.size = needs, size


class Work:
    def __init__(self, name, run, needs, cost):
        self.name, self.run, self.needs, self.cost = name, run, needs, cost


def up_from(k):
    if k == 4:
        return [("up", 0, 1, 4), ("up", 1, -1, 4)]
    way = 1 if k < 0 else -1
    return [("up", half, way, abs(k)) for half in range(2)]


def plan_copies():
    copies = {}

    def add(name, region, step, needs, size):
        copies[name] = Copy(name, region, step, tuple(needs), size)

    def reach(name, region, size, way):
        for d in (2, -2, 1, -1):
            add((*name, d), region(0), (0, 0, 0, d), (), size)
        for d in (3, -3):
            sign = d // 3
            add((*name, d), region(-2 * sign), (0, 0, 0, sign), [(*name, 2 * sign)], size)
        add((*name, 4), region(-2 * way), (0, 0, 0, 2 * way), [(*name, 2 * way)], size)

    def page(m):
        return lambda back: lambda r, x, y, c, z: r["w"].at[m, x, y, c, pl.ds(4 * ((z + back + NZ) % NZ), 4)]

    for m in range(3):
        reach(("page", m), page(m), 8, (1, -1, 1)[m])
    reach(("ub",), lambda back: lambda r, x, y, c, z: r["ub"].at[(z + back + NZ) % NZ], 4, -1)

    def ring(half, back):
        return lambda r, x, y, c, z: r["up"].at[(z + back + NZ) % NZ, c, pl.ds(32 * half, 32)]

    for s in range(1, 5):
        for half, way in ((0, 1), (1, -1), (1, 1), (0, -1)):
            if s == 4 and (half, way) in ((1, 1), (0, -1)):
                continue
            needs = [("up", half, way, s - 1)] if s > 1 else []
            add(("up", half, way, s), ring(half, -way * (s - 1)), (0, 0, 0, way), needs, 64)

    def hidden(src, dst, lo, rows):
        return lambda r, x, y, c, z: r["hb"].at[(z + src + NZ) % NZ, (z + dst + NZ) % NZ, pl.ds(lo, rows)]

    for sign in (1, -1):
        lo = 0 if sign == 1 else 64
        add(("hop", 4, lo), hidden(0, 4, lo, 64), (0, 0, 0, 2 * sign), ["h"], 16)
        add(("hop", 3 * sign), hidden(0, 3 * sign, 0, 128), (0, 0, 0, 2 * sign), ["h"], 32)
    for sign in (1, -1):
        for d in (2, 1):
            add(("hid", d * sign), hidden(0, d * sign, 0, 128), (0, 0, 0, d * sign), ["h"], 32)
    for sign in (1, -1):
        lo = 0 if sign == 1 else 64
        add(("hid", 3 * sign), hidden(-2 * sign, sign, 0, 128), (0, 0, 0, sign), [("hop", 3 * sign)], 32)
        add(("hid", 4, lo), hidden(-2 * sign, 2 * sign, lo, 64), (0, 0, 0, 2 * sign), [("hop", 4, lo)], 16)

    def whole(k):
        return lambda r, x, y, c, z: r["up"].at[(z + k + NZ) % NZ, c]

    for k in (-1, 1, -2, 2, -3, 3, 4):
        add(("pair", k), whole(k), (0, 0, 1, 0), up_from(k), 128)

    def block(m, h, i, j, lo, rows):
        def at(r, x, y, c, z):
            a, b = (x, y) if h == 0 else (y, x)
            a, b = (a + i + 4) % 4, (b + j + 4) % 4
            x, y = (a, b) if h == 0 else (b, a)
            return r["w"].at[m, x, y, c, pl.ds(16 * h + lo, rows)]

        return at

    def line(m, h, j, lo, rows):
        def at(r, x, y, c, z):
            if h == 0:
                return r["w"].at[m, :, (y + j + 4) % 4, c, pl.ds(16 * h + lo, rows)]
            return r["w"].at[m, (x + j + 4) % 4, :, c, pl.ds(16 * h + lo, rows)]

        return at

    for m in range(3):
        mine = [("page", m, d) for d in Z_STEPS]
        for h in range(2):
            along = (lambda d: (d, 0, 0, 0)) if h == 0 else (lambda d: (0, d, 0, 0))
            across = (lambda d: (0, d, 0, 0)) if h == 0 else (lambda d: (d, 0, 0, 0))
            key = (m, h)
            for d in (1, -1):
                add(("s1", key, d), block(m, h, 0, 0, 0, 16), along(d), mine, 32)
                add(("s3", key, 0, d), block(m, h, 0, 0, 0, 16), across(d), mine, 32)
            for d in (1, -1):
                lo = 0 if d == 1 else 8
                add(("s2", key, d), block(m, h, -d, 0, lo, 8), along(d), [("s1", key, d)], 16)
            for i in (-1, 1, 2):
                src = [("s1", key, -i)] if i != 2 else [("s2", key, 1), ("s2", key, -1)]
                for d in (1, -1):
                    add(("s3", key, i, d), block(m, h, i, 0, 0, 16), across(d), src, 32)
            for d in (1, -1):
                lo = 0 if d == 1 else 8
                got = [("s3", key, i, d) for i in (0, -1, 1, 2)]
                add(("s4", key, d), line(m, h, -d, lo, 8), across(d), got, 64)
            add(
                ("hand", key, 0),
                line(m, h, 0, 0, 16),
                (0, 0, 1, 0),
                mine + [("s1", key, 1), ("s1", key, -1), ("s2", key, 1), ("s2", key, -1)],
                128,
            )
            for d in (1, -1):
                got = [("s3", key, i, d) for i in (0, -1, 1, 2)]
                add(("hand", key, -d), line(m, h, -d, 0, 16), (0, 0, 1, 0), got, 128)
            for d in (1, -1):
                lo = 0 if d == 1 else 8
                add(("hand", key, 2, d), line(m, h, 2, lo, 8), (0, 0, 1, 0), [("s4", key, d)], 64)
    return copies


def all_of(m):
    names = [("page", m, d) for d in Z_STEPS]
    for h in range(2):
        key = (m, h)
        names += [("s1", key, d) for d in (1, -1)] + [("s2", key, d) for d in (1, -1)]
        names += [("s3", key, i, d) for i in (0, -1, 1, 2) for d in (1, -1)]
        names += [("s4", key, d) for d in (1, -1)]
        names += [("hand", key, j) for j in (0, 1, -1)] + [("hand", key, 2, d) for d in (1, -1)]
    return names


def pair_needs(k):
    if k == 0:
        return ["h"]
    hid = [("hid", 4, 0), ("hid", 4, 64)] if k == 4 else [("hid", -k)]
    return [("ub", 4 if k == 4 else -k), ("pair", k), *hid, *up_from(k)]


def urgency(name):
    kind = name[0]
    if kind == "page":
        return (0, name[1], 0)
    if kind in ("ub", "up", "hop", "hid", "pair"):
        return (1, {"hop": 0, "up": 1, "hid": 2, "ub": 3, "pair": 4}[kind], 0)
    return (2 + name[1][0], {"s1": 0, "s2": 1, "s3": 2, "s4": 3, "hand": 4}[kind], 0)


def plan_order(copies, works, backlog=2.0, margin=1.5):
    free, arrival, order = {}, {}, []
    now, waited, done = 0.0, set(), set()
    unsent, todo = sorted(copies, key=urgency), list(works)

    def route(c):
        axis = next(i for i in range(4) if c.step[i])
        hops = abs(c.step[axis])
        if axis == 2:
            return "core", c.size / 600.0, 0.9
        return (axis, c.step[axis] > 0), c.size * hops / 41.0, 0.95 + 0.8 * hops

    def start_ready(until):
        nonlocal now
        for name in list(unsent):
            c = copies[name]
            if all(n in waited or n in done for n in c.needs):
                link, took, late = route(c)
                if free.get(link, 0.0) - until > backlog:
                    continue
                begin = max(now, free.get(link, 0.0))
                free[link] = begin + took
                arrival[name] = begin + took + late
                order.append(("start", name))
                unsent.remove(name)
                now += 0.01

    feeds = {n for c in copies.values() for n in c.needs}

    def when(work):
        times = [0.0]
        for n in work.needs:
            if n in waited or n in done:
                continue
            if n in feeds or n not in arrival:
                return None
            times.append(arrival[n] + margin)
        return max(times)

    while True:
        start_ready(now)
        relays = sorted((arrival[n], i, n) for i, n in enumerate(arrival) if n in feeds and n not in waited)
        if relays and relays[0][0] <= now:
            order.append(("wait", relays[0][2]))
            waited.add(relays[0][2])
            continue
        times = [(when(w), i) for i, w in enumerate(todo) if when(w) is not None]
        run = next((i for t, i in times if t <= now), None)
        if run is None:
            following = [t for t, _ in times] + [t for t, _, _ in relays]
            if not following:
                break
            start_ready(min(following))
            now = max(now, min(following))
            continue
        run = todo.pop(run)
        for n in run.needs:
            if n in copies and n not in waited:
                order.append(("wait", n))
                waited.add(n)
        order.append(("work", run.name))
        now += run.cost
        done.add(run.name)
    assert not unsent and not todo
    order += [("wait", n) for n in copies if n not in waited]
    return order, now


def kernel(
    copies, tokens, dn_in, db_in, up_in, ub_in, q_in, k_in, v_in, out, xa, xs, w, dn, up, db, ub, hb, ad, qhl, qk, sc, mix, loc, ss, rs
):
    dp, z = lax.axis_index("dp"), lax.axis_index("adapter")
    x, y, c = dp // 8, (dp // 2) % 4, dp % 2
    refs = {"w": w, "up": up, "ub": ub, "hb": hb}
    ids = {name: i for i, name in enumerate(copies)}

    own = [
        (q_in, w.at[0, x, y, c, pl.ds(4 * z, 4)]),
        (k_in, w.at[1, x, y, c, pl.ds(4 * z, 4)]),
        (v_in, w.at[2, x, y, c, pl.ds(4 * z, 4)]),
        (ub_in, ub.at[z]),
        (up_in, up.at[z]),
        (db_in, db),
        (dn_in, dn),
        (tokens, xa),
        (tokens.at[pl.ds(128 * z, 128)], xs),
    ]
    own = [pltpu.make_async_copy(a, b, loc.at[i]) for i, (a, b) in enumerate(own)]
    for cp in own:
        cp.start()

    def there(step, sign):
        px, py, pz = (x + sign * step[0] + 4) % 4, (y + sign * step[1] + 4) % 4, (z + sign * step[3] + NZ) % NZ
        pc = 1 - c if step[2] else c
        return px, py, pc, pz

    def device(step):
        px, py, pc, pz = there(step, 1)
        return ((px * NY + py) * NC + pc, pz)

    def descriptor(name, sender):
        cp = copies[name]
        region = cp.region(refs, *sender)
        i = ids[name]
        return pltpu.make_async_remote_copy(
            src_ref=region,
            dst_ref=region,
            send_sem=ss.at[i],
            recv_sem=rs.at[i],
            device_id=device(cp.step),
            device_id_type=pl.DeviceIdType.MESH,
        )

    peers = [(0, 0, 0, d) for d in (1, -1, 2, -2)] + [(1, 0, 0, 0), (-1, 0, 0, 0), (0, 1, 0, 0), (0, -1, 0, 0), (0, 0, 1, 0)]
    barrier = pltpu.get_barrier_semaphore()
    for step in peers:
        pl.semaphore_signal(barrier, inc=1, device_id=device(step), device_id_type=pl.DeviceIdType.MESH)
    pl.semaphore_wait(barrier, len(peers))
    for cp in own[:5]:
        cp.wait()

    def hide():
        for cp in own[5:]:
            cp.wait()
        bias = db[...].astype(F32)
        bias = jnp.concatenate([bias[0:1], bias[1:2]], axis=1)
        both = dn.reshape(128, 1024)

        @pl.loop(0, NZ)
        def _(to):
            rows = xa[pl.ds(pl.multiple_of(to * 128, 128), 128), :]
            raised = lax.dot_general(rows, both[...], NT, preferred_element_type=F32)
            hb[z, to] = jnp.maximum(raised + bias, 0.0).astype(BF16)

    def adapters(k):
        def run():
            at = (z + k + NZ) % NZ
            hid = hb[at, z]
            lift = ub[at].astype(F32)
            for i in range(2):
                for n in range(4):
                    cols = slice(256 * n, 256 * n + 256)
                    raised = jnp.dot(hid[:, 64 * i : 64 * i + 64], up[at, i, :, cols], preferred_element_type=F32)
                    ad[2 * ((k + NZ) % NZ) + i, :, cols] = (
                        xs[:, cols].astype(F32) + raised + lift[i : i + 1, cols]
                    ).astype(BF16)

        return run

    def score(k):
        def run():
            first = 2 * ((k + NZ) % NZ)
            for a in (first, first + 1):
                total = ad[a, :, :128].astype(F32) * qk[:, :128]
                for n in range(1, 8):
                    cols = slice(128 * n, 128 * n + 128)
                    total = total + ad[a, :, cols].astype(F32) * qk[:, cols]
                sc[:, a : a + 1] = jnp.sum(total, axis=1, keepdims=True)

        return run

    def split(part, rows, cols, value):
        high = value.astype(BF16)
        part[rows, cols] = high
        low = slice(rows.start + 128, rows.stop + 128) if isinstance(rows, slice) else rows
        part[low, cols] = (value - high.astype(F32)).astype(BF16)

    def query():
        whole = w.at[0].reshape(1024, 1024)
        for n in range(4):
            cols = slice(256 * n, 256 * n + 256)
            split(qhl, slice(0, 128), cols, jnp.dot(xs[...], whole[:, cols], preferred_element_type=F32))

    def key():
        whole = w.at[1].reshape(1024, 1024)
        for n in range(4):
            cols = slice(256 * n, 256 * n + 256)
            both = lax.dot_general(qhl[...], whole[cols, :], NT, preferred_element_type=F32)
            qk[:, cols] = (both[:128] + both[128:]) * (1.0 / 32.0)

    def attend():
        weight = sc[:, :16]
        weight = jnp.exp(weight - jnp.max(weight, axis=1, keepdims=True))
        weight = weight / jnp.sum(weight, axis=1, keepdims=True)
        for row in range(0, 128, 16):
            rows = slice(row, row + 16)
            total = weight[rows, :1] * ad[0, rows, :].astype(F32)
            for a in range(1, 16):
                total = total + weight[rows, a : a + 1] * ad[a, rows, :].astype(F32)
            split(mix, rows, slice(None), total)

    def value():
        whole = w.at[2].reshape(1024, 1024)
        for n in range(4):
            cols = slice(256 * n, 256 * n + 256)
            both = jnp.dot(mix[...], whole[:, cols], preferred_element_type=F32)
            out[:, cols] = (xs[:, cols].astype(F32) + both[:128] + both[128:]).astype(BF16)

    pairs = [0, -1, 1, -2, 2, -3, 3, 4]
    works = [Work("h", hide, [], 1.3), Work("q", query, all_of(0), 0.6), Work("k", key, ["q"] + all_of(1), 0.8)]
    works += [Work(("a", k), adapters(k), pair_needs(k), 0.5) for k in pairs]
    works += [Work(("s", k), score(k), ["k", ("a", k)], 0.3) for k in pairs]
    works.append(Work("m", attend, [("s", k) for k in pairs], 1.5))
    works.append(Work("v", value, ["m"] + all_of(2), 0.8))
    by_name = {job.name: job for job in works}
    order, _ = plan_order(copies, works)
    for kind, name in order:
        if kind == "start":
            descriptor(name, (x, y, c, z)).start()
        elif kind == "wait":
            descriptor(name, there(copies[name].step, -1)).wait_recv()
        else:
            by_name[name].run()
    for name in copies:
        descriptor(name, (x, y, c, z)).wait_send()


def body(tokens, down_weight, down_bias, up_weight, up_bias, query_weight, key_weight, value_weight):
    copies = plan_copies()
    hbm = pl.BlockSpec(memory_space=pltpu.HBM)
    return pl.pallas_call(
        functools.partial(kernel, copies),
        out_shape=jax.ShapeDtypeStruct((128, 1024), BF16),
        in_specs=[hbm] * 8,
        out_specs=pl.BlockSpec(memory_space=pltpu.VMEM),
        scratch_shapes=[
            pltpu.VMEM((1024, 1024), BF16),
            pltpu.VMEM((128, 1024), BF16),
            pltpu.VMEM((3, NX, NY, NC, 32, 1024), BF16),
            pltpu.VMEM((2, 64, 1024), BF16),
            pltpu.VMEM((NZ, 2, 64, 1024), BF16),
            pltpu.VMEM((2, 64), BF16),
            pltpu.VMEM((NZ, 2, 1024), BF16),
            pltpu.VMEM((NZ, NZ, 128, 128), BF16),
            pltpu.VMEM((16, 128, 1024), BF16),
            pltpu.VMEM((256, 1024), BF16),
            pltpu.VMEM((128, 1024), F32),
            pltpu.VMEM((128, 16), F32),
            pltpu.VMEM((256, 1024), BF16),
            pltpu.SemaphoreType.DMA((9,)),
            pltpu.SemaphoreType.DMA((len(copies),)),
            pltpu.SemaphoreType.DMA((len(copies),)),
        ],
        compiler_params=pltpu.CompilerParams(
            collective_id=0, has_side_effects=True, vmem_limit_bytes=67043328
        ),
    )(
        tokens,
        jnp.swapaxes(down_weight, 1, 2),
        down_bias,
        up_weight,
        up_bias,
        query_weight,
        key_weight,
        value_weight,
    )


def solution(mesh):
    in_specs = (
        P("dp", None),
        P("adapter", None, None),
        P("adapter", None),
        P("adapter", None, None),
        P("adapter", None),
        P(("dp", "adapter"), None),
        P(("dp", "adapter"), None),
        P(("dp", "adapter"), None),
    )
    out_specs = P(("dp", "adapter"), None)
    return jax.shard_map(body, mesh=mesh, in_specs=in_specs, out_specs=out_specs, check_vma=False)
```

```python
import functools

import jax
import jax.numpy as jnp
from jax import lax
from jax.experimental import pallas as pl
from jax.experimental.pallas import tpu as pltpu
from jax.sharding import PartitionSpec as P

BF16, F32 = jnp.bfloat16, jnp.float32
NX, NY, NC, NZ = 4, 4, 2, 8
Z_STEPS = (4, 3, -3, 2, -2, 1, -1)
ORDER_Z = ("hop", "up", "hid", "ub", "pair")
ORDER_XY = ("s1", "s2", "s3", "s4", "hand")
MATRIX, MARGIN, BACKLOG, BACKLOG_Z = 10, 1.5, 2.0, 2.0
RATE, RATE_Z, LATE, COST = 41.0, 41.0, 0.95, 1.0
NT = (((1,), (1,)), ((), ()))


class Copy:
    def __init__(self, name, region, step, needs, size):
        self.name, self.region, self.step = name, region, step
        self.needs, self.size = needs, size


class Work:
    def __init__(self, name, run, needs, cost):
        self.name, self.run, self.needs, self.cost = name, run, needs, cost


def up_from(k):
    if k == 4:
        return [("up", 0, 1, 4), ("up", 1, -1, 4)]
    way = 1 if k < 0 else -1
    return [("up", half, way, abs(k)) for half in range(2)]


def plan_copies():
    copies = {}

    def add(name, region, step, needs, size):
        copies[name] = Copy(name, region, step, tuple(needs), size)

    def reach(name, region, size, way):
        for d in (2, -2, 1, -1):
            add((*name, d), region(0), (0, 0, 0, d), (), size)
        for d in (3, -3):
            sign = d // 3
            add((*name, d), region(-2 * sign), (0, 0, 0, sign), [(*name, 2 * sign)], size)
        add((*name, 4), region(-2 * way), (0, 0, 0, 2 * way), [(*name, 2 * way)], size)

    def page(m):
        return lambda back: lambda r, x, y, c, z: r["w"].at[m, x, y, c, pl.ds(4 * ((z + back + NZ) % NZ), 4)]

    for m in range(3):
        reach(("page", m), page(m), 8, (1, -1, 1)[m])
    reach(("ub",), lambda back: lambda r, x, y, c, z: r["ub"].at[(z + back + NZ) % NZ], 4, -1)

    def ring(half, back):
        return lambda r, x, y, c, z: r["up"].at[(z + back + NZ) % NZ, c, pl.ds(32 * half, 32)]

    for s in range(1, 5):
        for half, way in ((0, 1), (1, -1), (1, 1), (0, -1)):
            if s == 4 and (half, way) in ((1, 1), (0, -1)):
                continue
            needs = [("up", half, way, s - 1)] if s > 1 else []
            add(("up", half, way, s), ring(half, -way * (s - 1)), (0, 0, 0, way), needs, 64)

    def hidden(src, dst, lo, rows):
        return lambda r, x, y, c, z: r["hb"].at[(z + src + NZ) % NZ, (z + dst + NZ) % NZ, pl.ds(lo, rows)]

    for sign in (1, -1):
        lo = 0 if sign == 1 else 64
        add(("hop", 4, lo), hidden(0, 4, lo, 64), (0, 0, 0, 2 * sign), ["h"], 16)
        add(("hop", 3 * sign), hidden(0, 3 * sign, 0, 128), (0, 0, 0, 2 * sign), ["h"], 32)
    for sign in (1, -1):
        for d in (2, 1):
            add(("hid", d * sign), hidden(0, d * sign, 0, 128), (0, 0, 0, d * sign), ["h"], 32)
    for sign in (1, -1):
        lo = 0 if sign == 1 else 64
        add(("hid", 3 * sign), hidden(-2 * sign, sign, 0, 128), (0, 0, 0, sign), [("hop", 3 * sign)], 32)
        add(("hid", 4, lo), hidden(-2 * sign, 2 * sign, lo, 64), (0, 0, 0, 2 * sign), [("hop", 4, lo)], 16)

    def whole(k):
        return lambda r, x, y, c, z: r["up"].at[(z + k + NZ) % NZ, c]

    for k in (-1, 1, -2, 2, -3, 3, 4):
        add(("pair", k), whole(k), (0, 0, 1, 0), up_from(k), 128)

    def block(m, h, i, j, lo, rows):
        def at(r, x, y, c, z):
            a, b = (x, y) if h == 0 else (y, x)
            a, b = (a + i + 4) % 4, (b + j + 4) % 4
            x, y = (a, b) if h == 0 else (b, a)
            return r["w"].at[m, x, y, c, pl.ds(16 * h + lo, rows)]

        return at

    def line(m, h, j, lo, rows):
        def at(r, x, y, c, z):
            if h == 0:
                return r["w"].at[m, :, (y + j + 4) % 4, c, pl.ds(16 * h + lo, rows)]
            return r["w"].at[m, (x + j + 4) % 4, :, c, pl.ds(16 * h + lo, rows)]

        return at

    for m in range(3):
        mine = [("page", m, d) for d in Z_STEPS]
        for h in range(2):
            along = (lambda d: (d, 0, 0, 0)) if h == 0 else (lambda d: (0, d, 0, 0))
            across = (lambda d: (0, d, 0, 0)) if h == 0 else (lambda d: (d, 0, 0, 0))
            key = (m, h)
            for d in (1, -1):
                add(("s1", key, d), block(m, h, 0, 0, 0, 16), along(d), mine, 32)
                add(("s3", key, 0, d), block(m, h, 0, 0, 0, 16), across(d), mine, 32)
            for d in (1, -1):
                lo = 0 if d == 1 else 8
                add(("s2", key, d), block(m, h, -d, 0, lo, 8), along(d), [("s1", key, d)], 16)
            for i in (-1, 1, 2):
                src = [("s1", key, -i)] if i != 2 else [("s2", key, 1), ("s2", key, -1)]
                for d in (1, -1):
                    add(("s3", key, i, d), block(m, h, i, 0, 0, 16), across(d), src, 32)
            for d in (1, -1):
                lo = 0 if d == 1 else 8
                got = [("s3", key, i, d) for i in (0, -1, 1, 2)]
                add(("s4", key, d), line(m, h, -d, lo, 8), across(d), got, 64)
            add(
                ("hand", key, 0),
                line(m, h, 0, 0, 16),
                (0, 0, 1, 0),
                mine + [("s1", key, 1), ("s1", key, -1), ("s2", key, 1), ("s2", key, -1)],
                128,
            )
            for d in (1, -1):
                got = [("s3", key, i, d) for i in (0, -1, 1, 2)]
                add(("hand", key, -d), line(m, h, -d, 0, 16), (0, 0, 1, 0), got, 128)
            for d in (1, -1):
                lo = 0 if d == 1 else 8
                add(("hand", key, 2, d), line(m, h, 2, lo, 8), (0, 0, 1, 0), [("s4", key, d)], 64)
    return copies


def all_of(m):
    names = [("page", m, d) for d in Z_STEPS]
    for h in range(2):
        key = (m, h)
        names += [("s1", key, d) for d in (1, -1)] + [("s2", key, d) for d in (1, -1)]
        names += [("s3", key, i, d) for i in (0, -1, 1, 2) for d in (1, -1)]
        names += [("s4", key, d) for d in (1, -1)]
        names += [("hand", key, j) for j in (0, 1, -1)] + [("hand", key, 2, d) for d in (1, -1)]
    return names


def pair_needs(k):
    if k == 0:
        return ["h"]
    hid = [("hid", 4, 0), ("hid", 4, 64)] if k == 4 else [("hid", -k)]
    return [("ub", 4 if k == 4 else -k), ("pair", k), *hid, *up_from(k)]


def urgency(name):
    kind = name[0]
    if kind == "page":
        return (0, name[1], 0)
    if kind in ("ub", "up", "hop", "hid", "pair"):
        return (1, ORDER_Z.index(kind), 0)
    return (2, MATRIX * name[1][0] + ORDER_XY.index(kind), name[1][0])


def plan_order(copies, works, margin=MARGIN):
    free, arrival, order = {}, {}, []
    now, waited, done = 0.0, set(), set()
    unsent, todo = sorted(copies, key=urgency), list(works)

    def route(c):
        axis = next(i for i in range(4) if c.step[i])
        hops = abs(c.step[axis])
        if axis == 2:
            return "core", c.size / 600.0, 0.9
        return (axis, c.step[axis] > 0), c.size * hops / (RATE_Z if axis == 3 else RATE), LATE + 0.8 * hops

    def start_ready(until):
        nonlocal now
        for name in list(unsent):
            c = copies[name]
            if all(n in waited or n in done for n in c.needs):
                link, took, late = route(c)
                if free.get(link, 0.0) - until > (BACKLOG_Z if link[0] == 3 else BACKLOG):
                    continue
                begin = max(now, free.get(link, 0.0))
                free[link] = begin + took
                arrival[name] = begin + took + late
                order.append(("start", name))
                unsent.remove(name)
                now += 0.01

    feeds = {n for c in copies.values() for n in c.needs}

    def when(work):
        times = [0.0]
        for n in work.needs:
            if n in waited or n in done:
                continue
            if n in feeds or n not in arrival:
                return None
            times.append(arrival[n] + margin)
        return max(times)

    while True:
        start_ready(now)
        relays = sorted((arrival[n], i, n) for i, n in enumerate(arrival) if n in feeds and n not in waited)
        if relays and relays[0][0] <= now:
            order.append(("wait", relays[0][2]))
            waited.add(relays[0][2])
            continue
        times = [(when(w), i) for i, w in enumerate(todo) if when(w) is not None]
        run = next((i for t, i in times if t <= now), None)
        if run is None:
            following = [t for t, _ in times] + [t for t, _, _ in relays]
            if not following:
                break
            start_ready(min(following))
            now = max(now, min(following))
            continue
        run = todo.pop(run)
        for n in run.needs:
            if n in copies and n not in waited:
                order.append(("wait", n))
                waited.add(n)
        order.append(("work", run.name))
        now += run.cost * COST
        done.add(run.name)
    assert not unsent and not todo
    order += [("wait", n) for n in copies if n not in waited]
    return order, now


def kernel(
    copies, tokens, dn_in, db_in, up_in, ub_in, q_in, k_in, v_in, out, xa, xs, w, dn, up, db, ub, hb, ad, qhl, qk, sc, mix, loc, ss, rs
):
    dp, z = lax.axis_index("dp"), lax.axis_index("adapter")
    x, y, c = dp // 8, (dp // 2) % 4, dp % 2
    refs = {"w": w, "up": up, "ub": ub, "hb": hb}
    ids = {name: i for i, name in enumerate(copies)}

    own = [
        (q_in, w.at[0, x, y, c, pl.ds(4 * z, 4)]),
        (k_in, w.at[1, x, y, c, pl.ds(4 * z, 4)]),
        (v_in, w.at[2, x, y, c, pl.ds(4 * z, 4)]),
        (ub_in, ub.at[z]),
        (up_in, up.at[z]),
        (db_in, db),
        (dn_in, dn),
        (tokens, xa),
        (tokens.at[pl.ds(128 * z, 128)], xs),
    ]
    own = [pltpu.make_async_copy(a, b, loc.at[i]) for i, (a, b) in enumerate(own)]

    def there(step, sign):
        px, py, pz = (x + sign * step[0] + 4) % 4, (y + sign * step[1] + 4) % 4, (z + sign * step[3] + NZ) % NZ
        pc = 1 - c if step[2] else c
        return px, py, pc, pz

    def device(step):
        px, py, pc, pz = there(step, 1)
        return ((px * NY + py) * NC + pc, pz)

    def descriptor(name, sender):
        cp = copies[name]
        region = cp.region(refs, *sender)
        i = ids[name]
        return pltpu.make_async_remote_copy(
            src_ref=region,
            dst_ref=region,
            send_sem=ss.at[i],
            recv_sem=rs.at[i],
            device_id=device(cp.step),
            device_id_type=pl.DeviceIdType.MESH,
        )

    peers = [(0, 0, 0, d) for d in (1, -1, 2, -2)] + [(1, 0, 0, 0), (-1, 0, 0, 0), (0, 1, 0, 0), (0, -1, 0, 0), (0, 0, 1, 0)]
    barrier = pltpu.get_barrier_semaphore()
    for step in peers:
        pl.semaphore_signal(barrier, inc=1, device_id=device(step), device_id_type=pl.DeviceIdType.MESH)
    for cp in own:
        cp.start()
    pl.semaphore_wait(barrier, len(peers))
    sources = {("page", 0): 0, ("page", 1): 1, ("page", 2): 2, ("ub",): 3, ("up",): 4}

    def filled(name):
        for kind in (name[:1], name[:2]):
            if kind in sources:
                own[sources.pop(kind)].wait()


    def hide():
        for cp in own[5:]:
            cp.wait()
        bias = db[...].astype(F32)
        bias = jnp.concatenate([bias[0:1], bias[1:2]], axis=1)
        both = dn.reshape(128, 1024)

        @pl.loop(0, NZ)
        def _(to):
            rows = xa[pl.ds(pl.multiple_of(to * 128, 128), 128), :]
            raised = lax.dot_general(rows, both[...], NT, preferred_element_type=F32)
            hb[z, to] = jnp.maximum(raised + bias, 0.0).astype(BF16)

    def adapters(k):
        def run():
            at = (z + k + NZ) % NZ
            hid = hb[at, z]
            lift = ub[at].astype(F32)
            for i in range(2):
                for n in range(4):
                    cols = slice(256 * n, 256 * n + 256)
                    raised = jnp.dot(hid[:, 64 * i : 64 * i + 64], up[at, i, :, cols], preferred_element_type=F32)
                    ad[2 * ((k + NZ) % NZ) + i, :, cols] = (
                        xs[:, cols].astype(F32) + raised + lift[i : i + 1, cols]
                    ).astype(BF16)

        return run

    def score(k):
        def run():
            first = 2 * ((k + NZ) % NZ)
            for a in (first, first + 1):
                total = ad[a, :, :128].astype(F32) * qk[:, :128]
                for n in range(1, 8):
                    cols = slice(128 * n, 128 * n + 128)
                    total = total + ad[a, :, cols].astype(F32) * qk[:, cols]
                sc[:, a : a + 1] = jnp.sum(total, axis=1, keepdims=True)

        return run

    def split(part, rows, cols, value):
        high = value.astype(BF16)
        part[rows, cols] = high
        low = slice(rows.start + 128, rows.stop + 128) if isinstance(rows, slice) else rows
        part[low, cols] = (value - high.astype(F32)).astype(BF16)

    def query():
        whole = w.at[0].reshape(1024, 1024)
        for n in range(4):
            cols = slice(256 * n, 256 * n + 256)
            split(qhl, slice(0, 128), cols, jnp.dot(xs[...], whole[:, cols], preferred_element_type=F32))

    def key():
        whole = w.at[1].reshape(1024, 1024)
        for n in range(4):
            cols = slice(256 * n, 256 * n + 256)
            both = lax.dot_general(qhl[...], whole[cols, :], NT, preferred_element_type=F32)
            qk[:, cols] = (both[:128] + both[128:]) * (1.0 / 32.0)

    def attend():
        weight = sc[:, :16]
        weight = jnp.exp(weight - jnp.max(weight, axis=1, keepdims=True))
        weight = weight / jnp.sum(weight, axis=1, keepdims=True)
        for row in range(0, 128, 16):
            rows = slice(row, row + 16)
            total = weight[rows, :1] * ad[0, rows, :].astype(F32)
            for a in range(1, 16):
                total = total + weight[rows, a : a + 1] * ad[a, rows, :].astype(F32)
            split(mix, rows, slice(None), total)

    def value():
        whole = w.at[2].reshape(1024, 1024)
        for n in range(4):
            cols = slice(256 * n, 256 * n + 256)
            both = jnp.dot(mix[...], whole[:, cols], preferred_element_type=F32)
            out[:, cols] = (xs[:, cols].astype(F32) + both[:128] + both[128:]).astype(BF16)

    pairs = [0, -1, 1, -2, 2, -3, 3, 4]
    works = [Work("h", hide, [], 1.3), Work("q", query, all_of(0), 0.6), Work("k", key, ["q"] + all_of(1), 0.8)]
    works += [Work(("a", k), adapters(k), pair_needs(k), 0.5) for k in pairs]
    works += [Work(("s", k), score(k), ["k", ("a", k)], 0.3) for k in pairs]
    works.append(Work("m", attend, [("s", k) for k in pairs], 1.5))
    works.append(Work("v", value, ["m"] + all_of(2), 0.8))
    by_name = {job.name: job for job in works}
    order, _ = plan_order(copies, works)
    for kind, name in order:
        if kind == "start":
            filled(name)
            descriptor(name, (x, y, c, z)).start()
        elif kind == "wait":
            descriptor(name, there(copies[name].step, -1)).wait_recv()
        else:
            if name[0] == "a":
                filled(("ub",))
                filled(("up",))
            by_name[name].run()
    for name in copies:
        descriptor(name, (x, y, c, z)).wait_send()


def body(tokens, down_weight, down_bias, up_weight, up_bias, query_weight, key_weight, value_weight):
    copies = plan_copies()
    hbm = pl.BlockSpec(memory_space=pltpu.HBM)
    return pl.pallas_call(
        functools.partial(kernel, copies),
        out_shape=jax.ShapeDtypeStruct((128, 1024), BF16),
        in_specs=[hbm] * 8,
        out_specs=pl.BlockSpec(memory_space=pltpu.VMEM),
        scratch_shapes=[
            pltpu.VMEM((1024, 1024), BF16),
            pltpu.VMEM((128, 1024), BF16),
            pltpu.VMEM((3, NX, NY, NC, 32, 1024), BF16),
            pltpu.VMEM((2, 64, 1024), BF16),
            pltpu.VMEM((NZ, 2, 64, 1024), BF16),
            pltpu.VMEM((2, 64), BF16),
            pltpu.VMEM((NZ, 2, 1024), BF16),
            pltpu.VMEM((NZ, NZ, 128, 128), BF16),
            pltpu.VMEM((16, 128, 1024), BF16),
            pltpu.VMEM((256, 1024), BF16),
            pltpu.VMEM((128, 1024), F32),
            pltpu.VMEM((128, 16), F32),
            pltpu.VMEM((256, 1024), BF16),
            pltpu.SemaphoreType.DMA((9,)),
            pltpu.SemaphoreType.DMA((len(copies),)),
            pltpu.SemaphoreType.DMA((len(copies),)),
        ],
        compiler_params=pltpu.CompilerParams(
            collective_id=0, has_side_effects=True, vmem_limit_bytes=32 * 1024 * 1024
        ),
    )(
        *(
            pltpu.with_memory_space_constraint(a, pltpu.HBM)
            for a in (
                tokens,
                jnp.swapaxes(down_weight, 1, 2),
                down_bias,
                up_weight,
                up_bias,
                query_weight,
                key_weight,
                value_weight,
            )
        )
    )


def solution(mesh):
    in_specs = (
        P("dp", None),
        P("adapter", None, None),
        P("adapter", None),
        P("adapter", None, None),
        P("adapter", None),
        P(("dp", "adapter"), None),
        P(("dp", "adapter"), None),
        P(("dp", "adapter"), None),
    )
    out_specs = P(("dp", "adapter"), None)
    return jax.shard_map(body, mesh=mesh, in_specs=in_specs, out_specs=out_specs, check_vma=False)
```

```python
import functools

import jax
import jax.numpy as jnp
from jax import lax
from jax.experimental import pallas as pl
from jax.experimental.pallas import tpu as pltpu
from jax.sharding import PartitionSpec as P

BF16, F32 = jnp.bfloat16, jnp.float32
NX, NY, NC, NZ = 4, 4, 2, 8
Z_STEPS = (4, 3, -3, 2, -2, 1, -1)
ORDER_Z = ("hop", "up", "hid", "ub", "pair")
ORDER_XY = ("s1", "s2", "s4", "s3", "hand")
MATRIX, MARGIN, BACKLOG, BACKLOG_Z = 10, 1.0, 2.0, 2.0
RATE, RATE_Z, LATE, COST = 41.0, 41.0, 0.95, 0.6
NT = (((1,), (1,)), ((), ()))


class Copy:
    def __init__(self, name, region, step, needs, size):
        self.name, self.region, self.step = name, region, step
        self.needs, self.size = needs, size


class Work:
    def __init__(self, name, run, needs, cost):
        self.name, self.run, self.needs, self.cost = name, run, needs, cost


def up_from(k):
    if k == 4:
        return [("up", 0, 1, 4), ("up", 1, -1, 4)]
    way = 1 if k < 0 else -1
    return [("up", half, way, abs(k)) for half in range(2)]


def plan_copies():
    copies = {}

    def add(name, region, step, needs, size):
        copies[name] = Copy(name, region, step, tuple(needs), size)

    def reach(name, region, size, way):
        for d in (2, -2, 1, -1):
            add((*name, d), region(0), (0, 0, 0, d), (), size)
        for d in (3, -3):
            sign = d // 3
            add((*name, d), region(-2 * sign), (0, 0, 0, sign), [(*name, 2 * sign)], size)
        add((*name, 4), region(-2 * way), (0, 0, 0, 2 * way), [(*name, 2 * way)], size)

    def page(m):
        return lambda back: lambda r, x, y, c, z: r["w"].at[m, x, y, c, pl.ds(4 * ((z + back + NZ) % NZ), 4)]

    for m in range(3):
        reach(("page", m), page(m), 8, (1, -1, 1)[m])
    reach(("ub",), lambda back: lambda r, x, y, c, z: r["ub"].at[(z + back + NZ) % NZ], 4, -1)

    def ring(half, back):
        return lambda r, x, y, c, z: r["up"].at[(z + back + NZ) % NZ, c, pl.ds(32 * half, 32)]

    for s in range(1, 5):
        for half, way in ((0, 1), (1, -1), (1, 1), (0, -1)):
            if s == 4 and (half, way) in ((1, 1), (0, -1)):
                continue
            needs = [("up", half, way, s - 1)] if s > 1 else []
            add(("up", half, way, s), ring(half, -way * (s - 1)), (0, 0, 0, way), needs, 64)

    def hidden(src, dst, lo, rows):
        return lambda r, x, y, c, z: r["hb"].at[(z + src + NZ) % NZ, (z + dst + NZ) % NZ, pl.ds(lo, rows)]

    for sign in (1, -1):
        lo = 0 if sign == 1 else 64
        add(("hop", 4, lo), hidden(0, 4, lo, 64), (0, 0, 0, 2 * sign), ["h"], 16)
        add(("hop", 3 * sign), hidden(0, 3 * sign, 0, 128), (0, 0, 0, 2 * sign), ["h"], 32)
    for sign in (1, -1):
        for d in (2, 1):
            add(("hid", d * sign), hidden(0, d * sign, 0, 128), (0, 0, 0, d * sign), ["h"], 32)
    for sign in (1, -1):
        lo = 0 if sign == 1 else 64
        add(("hid", 3 * sign), hidden(-2 * sign, sign, 0, 128), (0, 0, 0, sign), [("hop", 3 * sign)], 32)
        add(("hid", 4, lo), hidden(-2 * sign, 2 * sign, lo, 64), (0, 0, 0, 2 * sign), [("hop", 4, lo)], 16)

    def whole(k):
        return lambda r, x, y, c, z: r["up"].at[(z + k + NZ) % NZ, c]

    for k in (-1, 1, -2, 2, -3, 3, 4):
        add(("pair", k), whole(k), (0, 0, 1, 0), up_from(k), 128)

    def block(m, h, i, j, lo, rows):
        def at(r, x, y, c, z):
            a, b = (x, y) if h == 0 else (y, x)
            a, b = (a + i + 4) % 4, (b + j + 4) % 4
            x, y = (a, b) if h == 0 else (b, a)
            return r["w"].at[m, x, y, c, pl.ds(16 * h + lo, rows)]

        return at

    def line(m, h, j, lo, rows):
        def at(r, x, y, c, z):
            if h == 0:
                return r["w"].at[m, :, (y + j + 4) % 4, c, pl.ds(16 * h + lo, rows)]
            return r["w"].at[m, (x + j + 4) % 4, :, c, pl.ds(16 * h + lo, rows)]

        return at

    for m in range(3):
        mine = [("page", m, d) for d in Z_STEPS]
        for h in range(2):
            along = (lambda d: (d, 0, 0, 0)) if h == 0 else (lambda d: (0, d, 0, 0))
            across = (lambda d: (0, d, 0, 0)) if h == 0 else (lambda d: (d, 0, 0, 0))
            key = (m, h)
            for d in (1, -1):
                add(("s1", key, d), block(m, h, 0, 0, 0, 16), along(d), mine, 32)
                add(("s3", key, 0, d), block(m, h, 0, 0, 0, 16), across(d), mine, 32)
            for d in (1, -1):
                lo = 0 if d == 1 else 8
                add(("s2", key, d), block(m, h, -d, 0, lo, 8), along(d), [("s1", key, d)], 16)
            for i in (-1, 1, 2):
                src = [("s1", key, -i)] if i != 2 else [("s2", key, 1), ("s2", key, -1)]
                for d in (1, -1):
                    add(("s3", key, i, d), block(m, h, i, 0, 0, 16), across(d), src, 32)
            for d in (1, -1):
                lo = 0 if d == 1 else 8
                got = [("s3", key, i, d) for i in (0, -1, 1, 2)]
                add(("s4", key, d), line(m, h, -d, lo, 8), across(d), got, 64)
            add(
                ("hand", key, 0),
                line(m, h, 0, 0, 16),
                (0, 0, 1, 0),
                mine + [("s1", key, 1), ("s1", key, -1), ("s2", key, 1), ("s2", key, -1)],
                128,
            )
            for d in (1, -1):
                got = [("s3", key, i, d) for i in (0, -1, 1, 2)]
                add(("hand", key, -d), line(m, h, -d, 0, 16), (0, 0, 1, 0), got, 128)
            for d in (1, -1):
                lo = 0 if d == 1 else 8
                add(("hand", key, 2, d), line(m, h, 2, lo, 8), (0, 0, 1, 0), [("s4", key, d)], 64)
    return copies


def all_of(m):
    names = [("page", m, d) for d in Z_STEPS]
    for h in range(2):
        key = (m, h)
        names += [("s1", key, d) for d in (1, -1)] + [("s2", key, d) for d in (1, -1)]
        names += [("s3", key, i, d) for i in (0, -1, 1, 2) for d in (1, -1)]
        names += [("s4", key, d) for d in (1, -1)]
        names += [("hand", key, j) for j in (0, 1, -1)] + [("hand", key, 2, d) for d in (1, -1)]
    return names


def pair_needs(k):
    if k == 0:
        return ["h"]
    hid = [("hid", 4, 0), ("hid", 4, 64)] if k == 4 else [("hid", -k)]
    return [("ub", 4 if k == 4 else -k), ("pair", k), *hid, *up_from(k)]


def urgency(name):
    kind = name[0]
    if kind == "page":
        return (0, name[1], 0)
    if kind in ("ub", "up", "hop", "hid", "pair"):
        return (1, ORDER_Z.index(kind), 0)
    return (2, MATRIX * name[1][0] + ORDER_XY.index(kind), name[1][0])


def plan_order(copies, works, margin=MARGIN):
    free, arrival, order = {}, {}, []
    now, waited, done = 0.0, set(), set()
    unsent, todo = sorted(copies, key=urgency), list(works)

    def route(c):
        axis = next(i for i in range(4) if c.step[i])
        hops = abs(c.step[axis])
        if axis == 2:
            return "core", c.size / 600.0, 0.9
        return (axis, c.step[axis] > 0), c.size * hops / (RATE_Z if axis == 3 else RATE), LATE + 0.8 * hops

    def start_ready(until):
        nonlocal now
        for name in list(unsent):
            c = copies[name]
            if all(n in waited or n in done for n in c.needs):
                link, took, late = route(c)
                if free.get(link, 0.0) - until > (BACKLOG_Z if link[0] == 3 else BACKLOG):
                    continue
                begin = max(now, free.get(link, 0.0))
                free[link] = begin + took
                arrival[name] = begin + took + late
                order.append(("start", name))
                unsent.remove(name)
                now += 0.01

    feeds = {n for c in copies.values() for n in c.needs}

    def when(work):
        times = [0.0]
        for n in work.needs:
            if n in waited or n in done:
                continue
            if n in feeds or n not in arrival:
                return None
            times.append(arrival[n] + margin)
        return max(times)

    while True:
        start_ready(now)
        relays = sorted((arrival[n], i, n) for i, n in enumerate(arrival) if n in feeds and n not in waited)
        if relays and relays[0][0] <= now:
            order.append(("wait", relays[0][2]))
            waited.add(relays[0][2])
            continue
        times = [(when(w), i) for i, w in enumerate(todo) if when(w) is not None]
        run = next((i for t, i in times if t <= now), None)
        if run is None:
            following = [t for t, _ in times] + [t for t, _, _ in relays]
            if not following:
                break
            start_ready(min(following))
            now = max(now, min(following))
            continue
        run = todo.pop(run)
        for n in run.needs:
            if n in copies and n not in waited:
                order.append(("wait", n))
                waited.add(n)
        order.append(("work", run.name))
        now += run.cost * COST
        done.add(run.name)
    assert not unsent and not todo
    order += [("wait", n) for n in copies if n not in waited]
    return order, now


def kernel(
    copies, tokens, dn_in, db_in, up_in, ub_in, q_in, k_in, v_in, out, xa, xs, w, dn, up, db, ub, hb, ad, qhl, qk, sc, mix, loc, ss, rs
):
    dp, z = lax.axis_index("dp"), lax.axis_index("adapter")
    x, y, c = dp // 8, (dp // 2) % 4, dp % 2
    refs = {"w": w, "up": up, "ub": ub, "hb": hb}
    ids = {name: i for i, name in enumerate(copies)}

    own = [
        (q_in, w.at[0, x, y, c, pl.ds(4 * z, 4)]),
        (k_in, w.at[1, x, y, c, pl.ds(4 * z, 4)]),
        (v_in, w.at[2, x, y, c, pl.ds(4 * z, 4)]),
        (ub_in, ub.at[z]),
        (up_in, up.at[z]),
        (db_in, db),
        (dn_in, dn),
        (tokens, xa),
        (tokens.at[pl.ds(128 * z, 128)], xs),
    ]
    own = [pltpu.make_async_copy(a, b, loc.at[i]) for i, (a, b) in enumerate(own)]

    def there(step, sign):
        px, py, pz = (x + sign * step[0] + 4) % 4, (y + sign * step[1] + 4) % 4, (z + sign * step[3] + NZ) % NZ
        pc = 1 - c if step[2] else c
        return px, py, pc, pz

    def device(step):
        px, py, pc, pz = there(step, 1)
        return ((px * NY + py) * NC + pc, pz)

    def descriptor(name, sender):
        cp = copies[name]
        region = cp.region(refs, *sender)
        i = ids[name]
        return pltpu.make_async_remote_copy(
            src_ref=region,
            dst_ref=region,
            send_sem=ss.at[i],
            recv_sem=rs.at[i],
            device_id=device(cp.step),
            device_id_type=pl.DeviceIdType.MESH,
        )

    peers = [(0, 0, 0, d) for d in (1, -1, 2, -2)] + [(1, 0, 0, 0), (-1, 0, 0, 0), (0, 1, 0, 0), (0, -1, 0, 0), (0, 0, 1, 0)]
    barrier = pltpu.get_barrier_semaphore()
    for step in peers:
        pl.semaphore_signal(barrier, inc=1, device_id=device(step), device_id_type=pl.DeviceIdType.MESH)
    for cp in own:
        cp.start()
    pl.semaphore_wait(barrier, len(peers))
    sources = {("page", 0): 0, ("page", 1): 1, ("page", 2): 2, ("ub",): 3, ("up",): 4}

    def filled(name):
        for kind in (name[:1], name[:2]):
            if kind in sources:
                own[sources.pop(kind)].wait()


    def hide():
        for cp in own[5:]:
            cp.wait()
        bias = db[...].astype(F32)
        bias = jnp.concatenate([bias[0:1], bias[1:2]], axis=1)
        both = dn.reshape(128, 1024)

        @pl.loop(0, NZ)
        def _(to):
            rows = xa[pl.ds(pl.multiple_of(to * 128, 128), 128), :]
            raised = lax.dot_general(rows, both[...], NT, preferred_element_type=F32)
            hb[z, to] = jnp.maximum(raised + bias, 0.0).astype(BF16)

    def adapters(k):
        def run():
            at = (z + k + NZ) % NZ
            hid = hb[at, z]
            lift = ub[at].astype(F32)
            for i in range(2):
                for n in range(4):
                    cols = slice(256 * n, 256 * n + 256)
                    raised = jnp.dot(hid[:, 64 * i : 64 * i + 64], up[at, i, :, cols], preferred_element_type=F32)
                    ad[2 * ((k + NZ) % NZ) + i, :, cols] = (
                        xs[:, cols].astype(F32) + raised + lift[i : i + 1, cols]
                    ).astype(BF16)

        return run

    def score(k):
        def run():
            first = 2 * ((k + NZ) % NZ)
            for a in (first, first + 1):
                total = ad[a, :, :128].astype(F32) * qk[:, :128]
                for n in range(1, 8):
                    cols = slice(128 * n, 128 * n + 128)
                    total = total + ad[a, :, cols].astype(F32) * qk[:, cols]
                sc[:, a : a + 1] = jnp.sum(total, axis=1, keepdims=True)

        return run

    def split(part, rows, cols, value):
        high = value.astype(BF16)
        part[rows, cols] = high
        low = slice(rows.start + 128, rows.stop + 128) if isinstance(rows, slice) else rows
        part[low, cols] = (value - high.astype(F32)).astype(BF16)

    def query():
        whole = w.at[0].reshape(1024, 1024)
        for n in range(4):
            cols = slice(256 * n, 256 * n + 256)
            split(qhl, slice(0, 128), cols, jnp.dot(xs[...], whole[:, cols], preferred_element_type=F32))

    def key():
        whole = w.at[1].reshape(1024, 1024)
        for n in range(4):
            cols = slice(256 * n, 256 * n + 256)
            both = lax.dot_general(qhl[...], whole[cols, :], NT, preferred_element_type=F32)
            qk[:, cols] = (both[:128] + both[128:]) * (1.0 / 32.0)

    def attend():
        weight = sc[:, :16]
        weight = jnp.exp(weight - jnp.max(weight, axis=1, keepdims=True))
        weight = weight / jnp.sum(weight, axis=1, keepdims=True)
        for row in range(0, 128, 16):
            rows = slice(row, row + 16)
            total = weight[rows, :1] * ad[0, rows, :].astype(F32)
            for a in range(1, 16):
                total = total + weight[rows, a : a + 1] * ad[a, rows, :].astype(F32)
            split(mix, rows, slice(None), total)

    def value():
        whole = w.at[2].reshape(1024, 1024)
        for n in range(4):
            cols = slice(256 * n, 256 * n + 256)
            both = jnp.dot(mix[...], whole[:, cols], preferred_element_type=F32)
            out[:, cols] = (xs[:, cols].astype(F32) + both[:128] + both[128:]).astype(BF16)

    pairs = [0, -1, 1, -2, 2, -3, 3, 4]
    works = [Work("h", hide, [], 1.3), Work("q", query, all_of(0), 0.6), Work("k", key, ["q"] + all_of(1), 0.8)]
    works += [Work(("a", k), adapters(k), pair_needs(k), 0.5) for k in pairs]
    works += [Work(("s", k), score(k), ["k", ("a", k)], 0.3) for k in pairs]
    works.append(Work("m", attend, [("s", k) for k in pairs], 1.5))
    works.append(Work("v", value, ["m"] + all_of(2), 0.8))
    by_name = {job.name: job for job in works}
    order, _ = plan_order(copies, works)
    for kind, name in order:
        if kind == "start":
            filled(name)
            descriptor(name, (x, y, c, z)).start()
        elif kind == "wait":
            descriptor(name, there(copies[name].step, -1)).wait_recv()
        else:
            if name[0] == "a":
                filled(("ub",))
                filled(("up",))
            by_name[name].run()
    for name in copies:
        descriptor(name, (x, y, c, z)).wait_send()


def body(tokens, down_weight, down_bias, up_weight, up_bias, query_weight, key_weight, value_weight):
    copies = plan_copies()
    hbm = pl.BlockSpec(memory_space=pltpu.HBM)
    return pl.pallas_call(
        functools.partial(kernel, copies),
        out_shape=jax.ShapeDtypeStruct((128, 1024), BF16),
        in_specs=[hbm] * 8,
        out_specs=pl.BlockSpec(memory_space=pltpu.VMEM),
        scratch_shapes=[
            pltpu.VMEM((1024, 1024), BF16),
            pltpu.VMEM((128, 1024), BF16),
            pltpu.VMEM((3, NX, NY, NC, 32, 1024), BF16),
            pltpu.VMEM((2, 64, 1024), BF16),
            pltpu.VMEM((NZ, 2, 64, 1024), BF16),
            pltpu.VMEM((2, 64), BF16),
            pltpu.VMEM((NZ, 2, 1024), BF16),
            pltpu.VMEM((NZ, NZ, 128, 128), BF16),
            pltpu.VMEM((16, 128, 1024), BF16),
            pltpu.VMEM((256, 1024), BF16),
            pltpu.VMEM((128, 1024), F32),
            pltpu.VMEM((128, 16), F32),
            pltpu.VMEM((256, 1024), BF16),
            pltpu.SemaphoreType.DMA((9,)),
            pltpu.SemaphoreType.DMA((len(copies),)),
            pltpu.SemaphoreType.DMA((len(copies),)),
        ],
        compiler_params=pltpu.CompilerParams(
            collective_id=0, has_side_effects=True, vmem_limit_bytes=32 * 1024 * 1024
        ),
    )(
        *(
            pltpu.with_memory_space_constraint(a, pltpu.HBM)
            for a in (
                tokens,
                jnp.swapaxes(down_weight, 1, 2),
                down_bias,
                up_weight,
                up_bias,
                query_weight,
                key_weight,
                value_weight,
            )
        )
    )


def solution(mesh):
    in_specs = (
        P("dp", None),
        P("adapter", None, None),
        P("adapter", None),
        P("adapter", None, None),
        P("adapter", None),
        P(("dp", "adapter"), None),
        P(("dp", "adapter"), None),
        P(("dp", "adapter"), None),
    )
    out_specs = P(("dp", "adapter"), None)
    return jax.shard_map(body, mesh=mesh, in_specs=in_specs, out_specs=out_specs, check_vma=False)
```
